128 devices in a mesh: group: 16 (over x, z_lo, core), head: 8 (over y, z_hi).
Axes of the slice: x: 4, y: 4, z: 4 (z_hi: 2, z_lo: 2; z = z_hi * 2 + z_lo), core: 2. Of those that a mesh axis runs over, the one named last changes fastest.
Arguments:
- hidden_in: bfloat16 [256, 2560], P('group'), may hold values from -6 to 6
- ssm_state: float32 [256, 80, 64, 128], P('group', 'head'), may hold values from -6 to 6
- conv_x_state: bfloat16 [256, 3, 5120], P('group', None, 'head'), may hold values from -6 to 6
- conv_bc_state: bfloat16 [256, 3, 256], P('group'), may hold values from -6 to 6
- token_ids: int32 [256], P('group'), may hold values from 0 to 25599
- ref_logits: bfloat16 [256, 25600], P('group', 'head'), may hold values from -15 to 350
- in_z: bfloat16 [2560, 5120], P('group', 'head'), may hold values from -0.125 to 0.125
- in_x: bfloat16 [2560, 5120], P('group', 'head'), may hold values from -0.125 to 0.125
- in_bc: bfloat16 [2560, 256], P('group'), may hold values from -0.125 to 0.125
- in_dt: bfloat16 [2560, 80], P('group', 'head'), may hold values from -0.125 to 0.125
- out_t: bfloat16 [2560, 5120], P('group', 'head'), may hold values from -0.078125 to 0.078125
- lm_head: bfloat16 [25600, 2560], P('head', 'group'), may hold values from -6 to 6
- conv_wx: float32 [4, 5120], P(None, 'head'), may hold values from -3 to 3
- conv_bx: float32 [5120], P('head'), may hold values from -1.5 to 1.5
- conv_wbc: float32 [4, 256], replicated, may hold values from -3 to 3
- conv_bbc: float32 [256], replicated, may hold values from -1.5 to 1.5
- dt_bias: float32 [80], P('head'), may hold values from -4 to -1
- a_log: float32 [80], P('head'), may hold values from 0 to 2.77
- skip_gain: float32 [80], P('head'), may hold values from 0.5 to 1.5
- norm_in: float32 [2560], replicated, may hold values from 0.5 to 1.5
- norm_gain: float32 [5120], P('head'), may hold values from 0.5 to 1.5
- final_gain: float32 [2560], replicated, may hold values from 0.5 to 1.5
Outputs:
- new_state: float32 [256, 80, 64, 128], P('group', 'head')
- divergence: float32 [256], P('group')
- token_logprob: float32 [256], P('group')
- roll_z: bfloat16 [2560, 5120], P(None, 'head')
- roll_x: bfloat16 [2560, 5120], P(None, 'head')
- roll_bc: bfloat16 [2560, 256], replicated
- roll_dt: bfloat16 [2560, 80], P(None, 'head')
- roll_out: bfloat16 [2560, 5120], P(None, 'head')
The draws below stay inside these ranges and needn't reach their ends.
All inputs are finite; a program needn't handle non-finite values.
Results may differ from the reference program's by a relative error of at most 0.0102.
Values may be sent and summed in bfloat16 or wider, within the bound.
No kernel may reach another device: no remote copies, remote signals or barrier semaphores. Data moves between devices by JAX's collectives and lax.ppermute only.
A program may use at most 128 MiB of HBM per device.

```python
import math
import jax
import jax.numpy as jnp
from jax import lax

D = 2560
H = 80
P_SIZE = 64
N = 128
KCONV = 4
V = 25600
SEQS = 16
DI = 5120
SEQ_ALL = 256
N_GROUP = 16


def draw_lm_head(key, part):
    subkeys = jax.random.split(key, 1)
    values = jax.random.normal(subkeys[0], (V, D), jnp.float32) * (3.0 / math.sqrt(D))
    return jnp.clip(values, -6.0, 6.0).astype(jnp.bfloat16)


def draw_ref_logits(key, part):
    subkeys = jax.random.split(key, 1)
    total_rows = SEQS * N_GROUP
    values = jnp.clip(jax.random.normal(subkeys[0], (total_rows, V), jnp.float32) * 3.0, -15.0, 15.0)
    return values.astype(jnp.bfloat16)


def place_ends(drawn, key, least, largest):
    place = [jax.random.randint(jax.random.fold_in(key, axis), (), 0, length) for axis, length in enumerate(drawn.shape)]
    longest = drawn.shape.index(max(drawn.shape))
    neighbour = place[:longest] + [(place[longest] + 1) % drawn.shape[longest]] + place[longest + 1:]
    return drawn.at[tuple(place)].set(least).at[tuple(neighbour)].set(largest)


def level_of(key, shape, pieces, smallest, top_value):
    level = 1.0
    for axis_at, shards_of in pieces:
        steps = jax.random.uniform(jax.random.fold_in(jax.random.fold_in(key, 6), axis_at), (shards_of,), jnp.float32, smallest / len(pieces), top_value / len(pieces))
        level = level * jnp.repeat(jnp.exp(steps), shape[axis_at] // shards_of).reshape((-1,) + (1,) * (len(shape) - 1 - axis_at))
    return level


def scatter_about(key, extent, scale, limit, pieces=(), held_as=jnp.bfloat16):
    entries = scale * jax.random.normal(key, extent, jnp.float32)
    if pieces:
        entries = entries * level_of(key, extent, pieces, -0.22, 0.18)
    return jnp.clip(entries, -limit, limit).astype(held_as)


def setup_inputs(seed: int = 0) -> dict:
    arg_keys = jax.random.split(jax.random.key(seed), 23)
    hidden_in = scatter_about(arg_keys[0], (SEQ_ALL, D), 1.0, 6.0, ((0, 16),))
    ssm_state = scatter_about(arg_keys[1], (SEQ_ALL, H, P_SIZE, N), 1.0, 6.0, ((0, 16), (1, 8)), jnp.float32)
    conv_x_state = scatter_about(arg_keys[2], (SEQ_ALL, KCONV - 1, DI), 1.0, 6.0, ((0, 16), (2, 8)))
    conv_bc_state = scatter_about(arg_keys[3], (SEQ_ALL, KCONV - 1, 2 * N), 1.0, 6.0, ((0, 16),))
    token_ids = place_ends(jax.random.randint(arg_keys[4], (SEQ_ALL,), 0, V), jax.random.fold_in(arg_keys[4], 1), 0, V - 1).astype(jnp.int32)
    ref_logits = draw_ref_logits(jax.random.fold_in(arg_keys[22], 71), 0)
    in_z = scatter_about(arg_keys[6], (D, DI), D ** -0.5, 0.125, ((0, 16), (1, 8)))
    in_x = scatter_about(arg_keys[7], (D, DI), D ** -0.5, 0.125, ((0, 16), (1, 8)))
    in_bc = scatter_about(arg_keys[8], (D, 2 * N), D ** -0.5, 0.125, ((0, 16),))
    in_dt = scatter_about(arg_keys[9], (D, H), D ** -0.5, 0.125, ((0, 16), (1, 8)))
    out_t = scatter_about(arg_keys[10], (D, DI), DI ** -0.5, 0.078125, ((0, 16), (1, 8)))
    lm_head = draw_lm_head(jax.random.fold_in(arg_keys[22], 71), 0)
    conv_wx = scatter_about(arg_keys[12], (KCONV, DI), KCONV ** -0.5, 3.0, ((1, 8),), jnp.float32)
    conv_bx = scatter_about(arg_keys[13], (DI,), 0.3, 1.5, ((0, 8),), jnp.float32)
    conv_wbc = scatter_about(arg_keys[14], (KCONV, 2 * N), KCONV ** -0.5, 3.0, (), jnp.float32)
    conv_bbc = scatter_about(arg_keys[15], (2 * N,), 0.3, 1.5, (), jnp.float32)
    dt_bias = jnp.clip(-4.0 + 3.0 * jax.random.uniform(arg_keys[16], (H,), jnp.float32) ** level_of(arg_keys[16], (H,), ((0, 8),), -0.2, 0.2), -4.0, -1.0)
    a_log = jnp.clip(2.77 * jax.random.uniform(arg_keys[17], (H,), jnp.float32) ** level_of(arg_keys[17], (H,), ((0, 8),), -0.2, 0.2), 0.0, 2.77)
    skip_gain = jnp.clip(0.5 + 1.0 * jax.random.uniform(arg_keys[18], (H,), jnp.float32) ** level_of(arg_keys[18], (H,), ((0, 8),), -0.2, 0.2), 0.5, 1.5)
    norm_in = jnp.clip(1.0 + 0.1 * jax.random.normal(arg_keys[19], (D,), jnp.float32), 0.5, 1.5)
    norm_gain = jnp.clip(1.0 + 0.1 * jax.random.normal(arg_keys[20], (DI,), jnp.float32), 0.5, 1.5)
    final_gain = jnp.clip(1.0 + 0.1 * jax.random.normal(arg_keys[21], (D,), jnp.float32), 0.5, 1.5)
    return {"hidden_in": hidden_in, "ssm_state": ssm_state, "conv_x_state": conv_x_state, "conv_bc_state": conv_bc_state, "token_ids": token_ids, "ref_logits": ref_logits, "in_z": in_z, "in_x": in_x, "in_bc": in_bc, "in_dt": in_dt, "out_t": out_t, "lm_head": lm_head, "conv_wx": conv_wx, "conv_bx": conv_bx, "conv_wbc": conv_wbc, "conv_bbc": conv_bbc, "dt_bias": dt_bias, "a_log": a_log, "skip_gain": skip_gain, "norm_in": norm_in, "norm_gain": norm_gain, "final_gain": final_gain}


EPSILON = 1e-05

def rms_norm(values, gain):
    return values * lax.rsqrt(lax.optimization_barrier(jnp.mean(values * values, axis=-1, keepdims=True)) + EPSILON) * gain

def causal_conv(history, newest, taps, offset):
    window = jnp.concatenate([history, newest[:, None, :]], axis=1).astype(jnp.float32)
    return jax.nn.silu(lax.optimization_barrier(jnp.sum(window * taps[None, :, :], axis=1)) + offset)

def reference(hidden_in, ssm_state, conv_x_state, conv_bc_state, token_ids, ref_logits, in_z, in_x, in_bc, in_dt, out_t, lm_head, conv_wx, conv_bx, conv_wbc, conv_bbc, dt_bias, a_log, skip_gain, norm_in, norm_gain, final_gain):
    stream_in = hidden_in.astype(jnp.float32)
    normed = rms_norm(stream_in, norm_in).astype(jnp.bfloat16)
    gate_branch = jnp.dot(normed, in_z, preferred_element_type=jnp.float32).astype(jnp.bfloat16)
    x_branch = jnp.dot(normed, in_x, preferred_element_type=jnp.float32).astype(jnp.bfloat16)
    bc_branch = jnp.dot(normed, in_bc, preferred_element_type=jnp.float32).astype(jnp.bfloat16)
    step_raw = jnp.dot(normed, in_dt, preferred_element_type=jnp.float32).astype(jnp.bfloat16)
    x_conv = causal_conv(conv_x_state, x_branch, conv_wx, conv_bx)
    bc_conv = causal_conv(conv_bc_state, bc_branch, conv_wbc, conv_bbc)
    b_vals = bc_conv[:, :N]
    c_vals = bc_conv[:, N:]
    step = jax.nn.softplus(step_raw.astype(jnp.float32) + dt_bias)
    decay = jnp.exp(-step * jnp.exp(a_log))
    seq_count = x_conv.shape[0]
    x_heads = x_conv.reshape(seq_count, H, P_SIZE)
    inflow = (step[:, :, None] * x_heads)[:, :, :, None] * b_vals[:, None, None, :]
    new_state = decay[:, :, None, None] * ssm_state + inflow
    ssm_out = jnp.einsum('shpn,sn->shp', new_state, c_vals, precision=lax.Precision.HIGHEST)
    ssm_out = (ssm_out + skip_gain[None, :, None] * x_heads).reshape(seq_count, H * P_SIZE)
    gated = ssm_out * jax.nn.silu(gate_branch.astype(jnp.float32))
    gated_out = rms_norm(gated, norm_gain).astype(jnp.bfloat16)
    mixed = lax.dot_general(gated_out, out_t, (((1,), (1,)), ((), ())), preferred_element_type=jnp.float32)
    final_hidden = rms_norm(stream_in + mixed, final_gain).astype(jnp.bfloat16)
    logits = lax.dot_general(final_hidden, lm_head, (((1,), (1,)), ((), ())), preferred_element_type=jnp.float32)
    lse_roll = jax.nn.logsumexp(logits, axis=-1)
    reference_rows = ref_logits.astype(jnp.float32)
    lse_ref = jax.nn.logsumexp(reference_rows, axis=-1)
    log_ref = reference_rows - lse_ref[:, None]
    divergence = lax.optimization_barrier(jnp.sum(jnp.exp(log_ref) * (log_ref - (logits - lse_roll[:, None])), axis=-1))
    picked = jnp.take_along_axis(logits, token_ids[:, None].astype(jnp.int32), axis=1)[:, 0]
    token_logprob = picked - lse_roll
    return (new_state, divergence, token_logprob, in_z, in_x, in_bc, in_dt, out_t)
```

```python
import jax
import jax.numpy as jnp
from jax import lax
from jax.sharding import Mesh
from jax.sharding import PartitionSpec as P

P_SIZE = 64
EPSILON = 1e-05
CHIPS = ("x", "z")
GROUP = ("x", "z", "core")
F32 = jnp.float32
BF16 = jnp.bfloat16


def from_partner(array):
    return lax.ppermute(array, "core", [(0, 1), (1, 0)])


def exchange(blocks, axis):
    return lax.all_to_all(blocks, axis, 0, 0, tiled=True)


def from_everyone(array, axis):
    peers = lax.axis_size(axis)
    return exchange(jnp.broadcast_to(array[None], (peers, *array.shape)), axis)


def two_parts(values):
    high = lax.reduce_precision(values, 8, 7)
    return high.astype(BF16), (values - high).astype(BF16)


def with_scalars(array, scalars):
    high, low = two_parts(scalars)
    spare = -(array.shape[-1] + 2) % 128
    tail = jnp.stack([high, low] + [jnp.zeros_like(high)] * spare, axis=-1)
    return jnp.concatenate([array, tail], axis=-1)


def conv_branch(history, newest, taps, offset):
    total = newest * taps[3] + offset
    for k in range(3):
        total = total + history[:, k, :].astype(F32) * taps[k]
    return jax.nn.silu(total)


def shards(
    hidden_in,
    ssm_state,
    conv_x_state,
    conv_bc_state,
    token_ids,
    ref_logits,
    in_z,
    in_x,
    in_bc,
    in_dt,
    out_t,
    lm_head,
    conv_wx,
    conv_bx,
    conv_wbc,
    conv_bbc,
    dt_bias,
    a_log,
    skip_gain,
    norm_in,
    norm_gain,
    final_gain,
):
    chips = lax.axis_size(CHIPS)
    first_core = lax.axis_index("core") == 0
    seqs, width = hidden_in.shape
    rows, inner = in_z.shape
    heads = a_log.shape[0]
    state_size = in_bc.shape[1] // 2
    class_seqs = chips * seqs

    dt_padded = jnp.pad(in_dt, ((0, 0), (0, -heads % 128)))
    own = jnp.concatenate([in_z, in_x, in_bc, dt_padded, out_t], axis=1)
    in_cols = own.shape[1] - inner
    gathered = lax.all_gather(own, GROUP, axis=0, tiled=True)
    roll_z = gathered[:, :inner]
    roll_x = gathered[:, inner : 2 * inner]
    roll_bc = gathered[:, 2 * inner : 2 * inner + 2 * state_size]
    dt_at = 2 * inner + 2 * state_size
    roll_dt = gathered[:, dt_at : dt_at + heads]
    roll_out = gathered[:, in_cols:]
    other = from_partner(own)
    lm_other = from_partner(lm_head)

    def own_first(array):
        left, right = array[:, :rows], array[:, rows:]
        return jnp.where(first_core, left, right), jnp.where(first_core, right, left)

    stream_in = hidden_in.astype(F32)
    scale = lax.rsqrt(jnp.mean(stream_in * stream_in, axis=-1, keepdims=True) + EPSILON)
    normed = (stream_in * scale * norm_in).astype(BF16)
    both = jnp.concatenate(
        [normed.reshape(seqs, chips, -1), hidden_in.reshape(seqs, chips, -1)], axis=-1
    ).transpose(1, 0, 2)
    both = exchange(both, CHIPS).reshape(class_seqs, -1)
    normed_own, normed_other = own_first(both[:, : 2 * rows])
    hidden_own, hidden_other = own_first(both[:, 2 * rows :])

    partial_in = jnp.dot(normed_own, own[:, :in_cols], preferred_element_type=F32) + jnp.dot(
        normed_other, other[:, :in_cols], preferred_element_type=F32
    )
    partial_in = exchange(partial_in.astype(BF16).reshape(chips, seqs, in_cols), CHIPS)
    branches = jnp.sum(partial_in.astype(F32), axis=0)
    gate = branches[:, :inner]
    x_conv = conv_branch(conv_x_state, branches[:, inner : 2 * inner], conv_wx, conv_bx)
    bc_conv = conv_branch(conv_bc_state, branches[:, 2 * inner : dt_at], conv_wbc, conv_bbc)
    b_vals, c_vals = bc_conv[:, :state_size], bc_conv[:, state_size:]
    step = jax.nn.softplus(branches[:, dt_at : dt_at + heads] + dt_bias)
    decay = jnp.exp(-step * jnp.exp(a_log))
    x_heads = x_conv.reshape(seqs, heads, P_SIZE)
    inflow = (step[:, :, None] * x_heads)[:, :, :, None] * b_vals[:, None, None, :]
    new_state = decay[:, :, None, None] * ssm_state + inflow
    carried = jnp.einsum("shpn,sn->shp", ssm_state, c_vals)
    overlap = jnp.sum(b_vals * c_vals, axis=-1)
    direct = step * overlap[:, None] + skip_gain
    ssm_out = (decay[:, :, None] * carried + direct[:, :, None] * x_heads).reshape(seqs, inner)
    gated = (ssm_out * jax.nn.silu(gate)).astype(BF16)

    gated = from_everyone(gated, CHIPS).reshape(class_seqs, inner).astype(F32)
    squares = jnp.sum(gated * gated, axis=-1)
    gained = (gated * norm_gain).astype(BF16)
    across = (((1,), (1,)), ((), ()))
    mix_own = lax.dot_general(gained, out_t, across, preferred_element_type=F32)
    mix_other = lax.dot_general(gained, other[:, in_cols:], across, preferred_element_type=F32)
    mix = jnp.concatenate([mix_own.astype(BF16), mix_other.astype(BF16)], axis=-1)
    mix = jnp.sum(from_everyone(with_scalars(mix, squares), "head").astype(F32), axis=0)
    square_total = mix[:, 2 * rows] + mix[:, 2 * rows + 1]
    mix_scale = lax.rsqrt(square_total / (inner * lax.axis_size("head")) + EPSILON)[:, None]
    stream_own = hidden_own.astype(F32) + mix_scale * mix[:, :rows]
    stream_other = hidden_other.astype(F32) + mix_scale * mix[:, rows : 2 * rows]

    group_at = lax.axis_index(GROUP)
    gain_own = lax.dynamic_slice_in_dim(final_gain, group_at * rows, rows)
    gain_other = lax.dynamic_slice_in_dim(final_gain, (group_at ^ 1) * rows, rows)
    squares = jnp.sum(stream_own * stream_own, axis=-1) + jnp.sum(stream_other * stream_other, axis=-1)
    partial_logits = lax.dot_general(
        (stream_own * gain_own).astype(BF16), lm_head, across, preferred_element_type=F32
    ) + lax.dot_general(
        (stream_other * gain_other).astype(BF16), lm_other, across, preferred_element_type=F32
    )
    vocab_local = lm_head.shape[0]
    sent = with_scalars(partial_logits.astype(BF16), squares).reshape(chips, seqs, -1)
    summed = jnp.sum(exchange(sent, CHIPS).astype(F32), axis=0)
    final_square = summed[:, vocab_local] + summed[:, vocab_local + 1]
    logits = summed[:, :vocab_local] * lax.rsqrt(final_square / width + EPSILON)[:, None]

    reference_rows = ref_logits.astype(F32)
    columns = lax.axis_index("head") * vocab_local + lax.broadcasted_iota(jnp.int32, (1, vocab_local), 1)
    picked = jnp.sum(jnp.where(columns == token_ids[:, None], logits, 0.0), axis=-1)
    roll_max = jnp.max(logits, axis=-1)
    ref_max = jnp.max(reference_rows, axis=-1)
    roll_sum = jnp.sum(jnp.exp(logits - roll_max[:, None]), axis=-1)
    ref_weights = jnp.exp(reference_rows - ref_max[:, None])
    ref_sum = jnp.sum(ref_weights, axis=-1)
    cross_sum = jnp.sum(ref_weights * (reference_rows - logits), axis=-1)
    zero = jnp.zeros_like(picked)
    stats = jnp.stack([roll_max, roll_sum, ref_max, ref_sum, cross_sum, picked, zero, zero])
    stats = from_everyone(stats, "head")
    roll_top = jnp.max(stats[:, 0], axis=0)
    ref_top = jnp.max(stats[:, 2], axis=0)
    roll_total = jnp.sum(stats[:, 1] * jnp.exp(stats[:, 0] - roll_top), axis=0)
    ref_scale = jnp.exp(stats[:, 2] - ref_top)
    ref_total = jnp.sum(stats[:, 3] * ref_scale, axis=0)
    cross_total = jnp.sum(stats[:, 4] * ref_scale, axis=0)
    lse_roll = roll_top + jnp.log(roll_total)
    lse_ref = ref_top + jnp.log(ref_total)
    divergence = cross_total / ref_total - lse_ref + lse_roll
    token_logprob = jnp.sum(stats[:, 5], axis=0) - lse_roll
    return (new_state, divergence, token_logprob, roll_z, roll_x, roll_bc, roll_dt, roll_out)


def solution(mesh):
    group, head = mesh.devices.shape
    fine = Mesh(mesh.devices.reshape(group // 4, 2, 2, head), ("x", "z", "core", "head"))
    return jax.shard_map(
        shards,
        mesh=fine,
        in_specs=(
            P(GROUP, None),
            P(GROUP, "head", None, None),
            P(GROUP, None, "head"),
            P(GROUP, None, None),
            P(GROUP),
            P(GROUP, "head"),
            P(GROUP, "head"),
            P(GROUP, "head"),
            P(GROUP, None),
            P(GROUP, "head"),
            P(GROUP, "head"),
            P("head", GROUP),
            P(None, "head"),
            P("head"),
            P(),
            P(),
            P("head"),
            P("head"),
            P("head"),
            P(),
            P("head"),
            P(),
        ),
        out_specs=(
            P(GROUP, "head", None, None),
            P(GROUP),
            P(GROUP),
            P(None, "head"),
            P(None, "head"),
            P(),
            P(None, "head"),
            P(None, "head"),
        ),
        check_vma=False,
    )
```

```python
import functools

import jax
import jax.numpy as jnp
from jax import lax
from jax.experimental import pallas as pl
from jax.experimental.pallas import tpu as pltpu
from jax.sharding import Mesh
from jax.sharding import PartitionSpec as P

P_SIZE = 64
EPSILON = 1e-05
CHIPS = ("x", "z")
GROUP = ("x", "z", "core")
F32 = jnp.float32
BF16 = jnp.bfloat16


def from_partner(array):
    return lax.ppermute(array, "core", [(0, 1), (1, 0)])


def from_opposite(array):
    return lax.ppermute(array, "z", [(0, 1), (1, 0)])


def along_ring(array, sign):
    ring = lax.axis_size("x")
    pairs = [
        (2 * x + core, 2 * ((x + (sign if core == 0 else -sign)) % ring) + core)
        for x in range(ring)
        for core in range(2)
    ]
    return lax.ppermute(array, ("x", "core"), pairs)


def joined_kernel(in_z, in_x, in_bc, in_dt, out_t, own):
    at = 0
    for part in (in_z, in_x, in_bc):
        own[:, at : at + part.shape[1]] = part[...]
        at += part.shape[1]
    own[:, at : at + 128] = jnp.zeros((own.shape[0], 128), own.dtype)
    own[:, at : at + in_dt.shape[1]] = in_dt[...]
    own[:, at + 128 :] = out_t[...]


def joined(in_z, in_x, in_bc, in_dt, out_t):
    rows, inner = in_z.shape
    whole = 3 * inner + in_bc.shape[1] + 128
    return pl.pallas_call(
        joined_kernel,
        out_shape=jax.ShapeDtypeStruct((rows, whole), in_z.dtype),
        cost_estimate=pl.CostEstimate(flops=2000000, bytes_accessed=2 * 2 * rows * whole, transcendentals=0),
    )(in_z, in_x, in_bc, in_dt, out_t)


def blocks_kernel(hidden, gain, out, scale):
    values = hidden[...].astype(F32)
    mean = jnp.mean(values * values, axis=-1, keepdims=True)
    scale[...] = jnp.broadcast_to(lax.rsqrt(mean + EPSILON), scale.shape)
    gained = (values * gain[...]).astype(out.dtype)
    wide = out.shape[2] // 2
    for k in range(out.shape[0]):
        out[k, :, :wide] = gained[:, k * wide : (k + 1) * wide]
        out[k, :, wide:] = hidden[:, k * wide : (k + 1) * wide]


def hidden_blocks(hidden, gain, chips):
    seqs, width = hidden.shape
    return pl.pallas_call(
        blocks_kernel,
        out_shape=(
            jax.ShapeDtypeStruct((chips, seqs, 2 * width // chips), hidden.dtype),
            jax.ShapeDtypeStruct((seqs, 128), F32),
        ),
        cost_estimate=pl.CostEstimate(flops=1000000, bytes_accessed=300000, transcendentals=0),
    )(hidden, gain.reshape(1, width))


def placed_kernel(tags, widths, *refs):
    count = len(tags)
    pieces = refs[:count]
    outs, (held, in_sems, out_sems) = refs[-len(widths) - 3 : -3], refs[-3:]
    rows = pieces[0].shape[0]
    x, z, core = (lax.axis_index(name) for name in ("x", "z", "core"))
    reads = [pltpu.make_async_copy(pieces[i], held.at[i], in_sems.at[i]) for i in range(count)]
    for read in reads:
        read.start()
    writes = []
    for i, (turn, over, swap) in enumerate(tags):
        source_core = lax.rem(core + swap, 2)
        back = lax.rem(4 - turn + turn * 2 * source_core, 4)
        source = lax.rem(x + back, 4) * 4 + lax.rem(z + over, 2) * 2 + source_core
        at = pl.multiple_of(source * rows, rows)
        reads[i].wait()
        col = 0
        for j, wide in enumerate(widths):
            write = pltpu.make_async_copy(
                held.at[i, :, pl.ds(col, wide)],
                outs[j].at[pl.ds(at, rows), :],
                out_sems.at[i, j],
            )
            write.start()
            writes.append(write)
            col += wide
    for write in writes:
        write.wait()


def placed(pieces, devices, widths, earlier=()):
    tags, arrays = list(pieces), list(pieces.values())
    rows, whole = arrays[0].shape
    count = len(tags)
    anywhere = pl.BlockSpec(memory_space=pl.ANY)
    return pl.pallas_call(
        functools.partial(placed_kernel, tags, widths),
        out_shape=tuple(jax.ShapeDtypeStruct((rows * devices, wide), arrays[0].dtype) for wide in widths),
        in_specs=[anywhere] * (count + len(earlier)),
        out_specs=tuple(anywhere for _ in widths),
        scratch_shapes=[
            pltpu.VMEM((count, rows, whole), arrays[0].dtype),
            pltpu.SemaphoreType.DMA((count,)),
            pltpu.SemaphoreType.DMA((count, len(widths))),
        ],
        input_output_aliases={count + j: j for j in range(len(earlier))},
        compiler_params=pltpu.CompilerParams(vmem_limit_bytes=12 * 2**20),
        cost_estimate=pl.CostEstimate(flops=10000000, bytes_accessed=4 * count * rows * whole, transcendentals=0),
    )(*arrays, *earlier)


def exchange(blocks, axis):
    return lax.all_to_all(blocks, axis, 0, 0, tiled=True)


def from_everyone(array, axis):
    peers = lax.axis_size(axis)
    return exchange(jnp.broadcast_to(array[None], (peers, *array.shape)), axis)


def two_parts(values):
    high = lax.reduce_precision(values, 8, 7)
    return high.astype(BF16), (values - high).astype(BF16)


def with_scalars(array, scalars):
    high, low = two_parts(scalars)
    spare = -(array.shape[-1] + 2) % 128
    tail = jnp.stack([high, low] + [jnp.zeros_like(high)] * spare, axis=-1)
    return jnp.concatenate([array, tail], axis=-1)


def column(index, values, lanes):
    return jnp.where(lax.broadcasted_iota(jnp.int32, (values.shape[0], lanes), 1) == index, values, 0.0)


def logits_kernel(inner_total, mixed, both, gains, lm_own, lm_other, out):
    rows = lm_own.shape[0]
    vocab = lm_own.shape[1]
    core = lax.axis_index("core")
    at = lax.axis_index("x") * 4 + lax.axis_index("z") * 2 + core
    total = mixed[0].astype(F32)
    for k in range(1, mixed.shape[0]):
        total = total + mixed[k].astype(F32)
    square = total[:, 2 * rows : 2 * rows + 1] + total[:, 2 * rows + 1 : 2 * rows + 2]
    scale = lax.rsqrt(square / inner_total + EPSILON)
    left = both[:, 2 * rows : 3 * rows].astype(F32)
    right = both[:, 3 * rows : 4 * rows].astype(F32)
    stream_own = jnp.where(core == 0, left, right) + scale * total[:, :rows]
    stream_other = jnp.where(core == 0, right, left) + scale * total[:, rows : 2 * rows]
    squares = jnp.sum(stream_own * stream_own, axis=-1, keepdims=True) + jnp.sum(
        stream_other * stream_other, axis=-1, keepdims=True
    )
    final_own = (stream_own * gains[pl.ds(at, 1), :]).astype(BF16)
    final_other = (stream_other * gains[pl.ds(at + 1 - 2 * core, 1), :]).astype(BF16)
    wide = 640
    for start in range(0, vocab, wide):
        part = jnp.dot(final_own, lm_own[:, start : start + wide], preferred_element_type=F32)
        part = part + jnp.dot(final_other, lm_other[:, start : start + wide], preferred_element_type=F32)
        out[:, start : start + wide] = part.astype(BF16)
    high = squares.astype(BF16).astype(F32)
    out[:, vocab:] = (column(0, high, 128) + column(1, squares - high, 128)).astype(BF16)


def partial_logits(mixed, both, gains, lm_own, lm_other, inner_total):
    _, vocab = lm_own.shape
    return pl.pallas_call(
        functools.partial(logits_kernel, inner_total),
        out_shape=jax.ShapeDtypeStruct((both.shape[0], vocab + 128), BF16),
        compiler_params=pltpu.CompilerParams(vmem_limit_bytes=24 * 2**20),
        cost_estimate=pl.CostEstimate(flops=300000000, bytes_accessed=4000000, transcendentals=0),
    )(mixed, both, gains, lm_own, lm_other)


def stats_kernel(width, parts, reference, tokens, out):
    vocab = reference.shape[1]
    total = parts[0].astype(F32)
    for k in range(1, parts.shape[0]):
        total = total + parts[k].astype(F32)
    square = total[:, vocab : vocab + 1] + total[:, vocab + 1 : vocab + 2]
    logits = total[:, :vocab] * lax.rsqrt(square / width + EPSILON)
    rows = reference[...].astype(F32)
    columns = lax.axis_index("head") * vocab + lax.broadcasted_iota(jnp.int32, logits.shape, 1)
    picked = jnp.sum(jnp.where(columns == tokens[...], logits, 0.0), axis=-1, keepdims=True)
    roll_max = jnp.max(logits, axis=-1, keepdims=True)
    ref_max = jnp.max(rows, axis=-1, keepdims=True)
    roll_sum = jnp.sum(jnp.exp(logits - roll_max), axis=-1, keepdims=True)
    weights = jnp.exp(rows - ref_max)
    ref_sum = jnp.sum(weights, axis=-1, keepdims=True)
    cross = jnp.sum(weights * (rows - logits), axis=-1, keepdims=True)
    found = column(0, roll_max, 128)
    for index, values in enumerate((roll_sum, ref_max, ref_sum, cross, picked), 1):
        found = found + column(index, values, 128)
    turned = found.T[:8]
    for k in range(out.shape[0]):
        out[k, :, : turned.shape[1]] = turned
        out[k, :, turned.shape[1] :] = jnp.zeros((8, 128 - turned.shape[1]), F32)


def head_stats(parts, reference, tokens, width, peers):
    return pl.pallas_call(
        functools.partial(stats_kernel, width),
        out_shape=jax.ShapeDtypeStruct((peers, 8, 128), F32),
        compiler_params=pltpu.CompilerParams(vmem_limit_bytes=16 * 2**20),
        cost_estimate=pl.CostEstimate(flops=3000000, bytes_accessed=1000000, transcendentals=100000),
    )(parts, reference, tokens)


def combine_kernel(stats, divergence, logprob):
    rows = [[stats[k, j : j + 1, :] for j in range(6)] for k in range(stats.shape[0])]
    roll_top, ref_top = rows[0][0], rows[0][2]
    for row in rows[1:]:
        roll_top, ref_top = jnp.maximum(roll_top, row[0]), jnp.maximum(ref_top, row[2])
    roll_total = sum(row[1] * jnp.exp(row[0] - roll_top) for row in rows)
    scales = [jnp.exp(row[2] - ref_top) for row in rows]
    ref_total = sum(row[3] * scale for row, scale in zip(rows, scales))
    cross_total = sum(row[4] * scale for row, scale in zip(rows, scales))
    lse_roll = roll_top + jnp.log(roll_total)
    lse_ref = ref_top + jnp.log(ref_total)
    count = divergence.shape[1]
    divergence[...] = (cross_total / ref_total - lse_ref + lse_roll)[:, :count]
    logprob[...] = (sum(row[5] for row in rows) - lse_roll)[:, :count]


def combined(stats, seqs):
    return pl.pallas_call(
        combine_kernel,
        out_shape=(jax.ShapeDtypeStruct((1, seqs), F32),) * 2,
        cost_estimate=pl.CostEstimate(flops=100000, bytes_accessed=40000, transcendentals=0),
    )(stats)


def conv_branch(history, newest, taps, offset):
    total = newest * taps[3] + offset
    for k in range(3):
        total = total + history[:, k, :].astype(F32) * taps[k]
    return jax.nn.silu(total)


def shards(
    hidden_in,
    ssm_state,
    conv_x_state,
    conv_bc_state,
    token_ids,
    ref_logits,
    in_z,
    in_x,
    in_bc,
    in_dt,
    out_t,
    lm_head,
    conv_wx,
    conv_bx,
    conv_wbc,
    conv_bbc,
    dt_bias,
    a_log,
    skip_gain,
    norm_in,
    norm_gain,
    final_gain,
):
    chips = lax.axis_size(CHIPS)
    first_core = lax.axis_index("core") == 0
    seqs, width = hidden_in.shape
    rows, inner = in_z.shape
    heads = a_log.shape[0]
    state_size = in_bc.shape[1] // 2
    class_seqs = chips * seqs

    hidden_sent, scale = hidden_blocks(hidden_in, norm_in, chips)
    own = joined(in_z, in_x, in_bc, in_dt, out_t)
    in_cols = own.shape[1] - inner
    dt_at = 2 * inner + 2 * state_size
    other = from_partner(own)
    ahead = along_ring(own, 1)
    behind = along_ring(own, -1)
    over = from_opposite(own)
    lm_other = from_partner(lm_head)
    far = along_ring(ahead, 1)
    ahead_z = along_ring(over, 1)
    behind_z = along_ring(over, -1)
    far_z = along_ring(ahead_z, 1)
    pieces = {(0, 0, 0): own, (0, 0, 1): other}
    for at, piece in (
        ((0, 1), over),
        ((1, 0), ahead),
        ((3, 0), behind),
        ((1, 1), ahead_z),
        ((3, 1), behind_z),
        ((2, 0), far),
        ((2, 1), far_z),
    ):
        pieces.update({(*at, 0): piece, (*at, 1): from_partner(piece)})
    widths = (inner, inner, 2 * state_size, 128, inner)
    first, second = list(pieces)[:8], list(pieces)[8:]
    devices = 2 * chips
    rolled = placed({tag: pieces[tag] for tag in first}, devices, widths)
    rolled = placed({tag: pieces[tag] for tag in second}, devices, widths, rolled)
    roll_z, roll_x, roll_bc, dt_wide, roll_out = rolled
    roll_dt = dt_wide[:, :heads]

    def own_first(array):
        left, right = array[:, :rows], array[:, rows:]
        return jnp.where(first_core, left, right), jnp.where(first_core, right, left)

    both = exchange(hidden_sent, CHIPS)
    both = both.reshape(class_seqs, -1)
    normed_own, normed_other = own_first(both[:, : 2 * rows])

    partial_in = jnp.dot(normed_own, own[:, :in_cols], preferred_element_type=F32) + jnp.dot(
        normed_other, other[:, :in_cols], preferred_element_type=F32
    )
    partial_in = partial_in.astype(BF16).reshape(chips, seqs, in_cols)
    partial_in = exchange(partial_in, CHIPS)
    branches = jnp.sum(partial_in.astype(F32), axis=0) * scale[:, :1]
    gate = branches[:, :inner]
    x_conv = conv_branch(conv_x_state, branches[:, inner : 2 * inner], conv_wx, conv_bx)
    bc_conv = conv_branch(conv_bc_state, branches[:, 2 * inner : dt_at], conv_wbc, conv_bbc)
    b_vals, c_vals = bc_conv[:, :state_size], bc_conv[:, state_size:]
    step = jax.nn.softplus(branches[:, dt_at : dt_at + heads] + dt_bias)
    decay = jnp.exp(-step * jnp.exp(a_log))
    x_heads = x_conv.reshape(seqs, heads, P_SIZE)
    inflow = (step[:, :, None] * x_heads)[:, :, :, None] * b_vals[:, None, None, :]
    new_state = decay[:, :, None, None] * ssm_state + inflow
    carried = jnp.einsum("shpn,sn->shp", ssm_state, c_vals)
    overlap = jnp.sum(b_vals * c_vals, axis=-1)
    direct = step * overlap[:, None] + skip_gain
    ssm_out = (decay[:, :, None] * carried + direct[:, :, None] * x_heads).reshape(seqs, inner)
    gated = (ssm_out * jax.nn.silu(gate)).astype(BF16)

    gated = from_everyone(gated, CHIPS)
    gated = gated.reshape(class_seqs, inner).astype(F32)
    squares = jnp.sum(gated * gated, axis=-1)
    gained = (gated * norm_gain).astype(BF16)
    across = (((1,), (1,)), ((), ()))
    mix_own = lax.dot_general(gained, out_t, across, preferred_element_type=F32)
    mix_other = lax.dot_general(gained, other[:, in_cols:], across, preferred_element_type=F32)
    mix = jnp.concatenate([mix_own.astype(BF16), mix_other.astype(BF16)], axis=-1)
    mix = with_scalars(mix, squares)
    mix = from_everyone(mix, "head")

    sent = partial_logits(
        mix, both, final_gain.reshape(-1, rows), lm_head.T, lm_other.T, inner * lax.axis_size("head")
    )
    parts = exchange(sent.reshape(chips, seqs, -1), CHIPS)
    stats = head_stats(parts, ref_logits, token_ids[:, None], width, lax.axis_size("head"))
    stats = exchange(stats, "head")
    divergence, token_logprob = combined(stats, seqs)
    divergence, token_logprob = divergence[0], token_logprob[0]
    return (new_state, divergence, token_logprob, roll_z, roll_x, roll_bc, roll_dt, roll_out)


def solution(mesh):
    group, head = mesh.devices.shape
    fine = Mesh(mesh.devices.reshape(group // 4, 2, 2, head), ("x", "z", "core", "head"))
    return jax.shard_map(
        shards,
        mesh=fine,
        in_specs=(
            P(GROUP, None),
            P(GROUP, "head", None, None),
            P(GROUP, None, "head"),
            P(GROUP, None, None),
            P(GROUP),
            P(GROUP, "head"),
            P(GROUP, "head"),
            P(GROUP, "head"),
            P(GROUP, None),
            P(GROUP, "head"),
            P(GROUP, "head"),
            P("head", GROUP),
            P(None, "head"),
            P("head"),
            P(),
            P(),
            P("head"),
            P("head"),
            P("head"),
            P(),
            P("head"),
            P(),
        ),
        out_specs=(
            P(GROUP, "head", None, None),
            P(GROUP),
            P(GROUP),
            P(None, "head"),
            P(None, "head"),
            P(),
            P(None, "head"),
            P(None, "head"),
        ),
        check_vma=False,
    )
```

```python
import functools

import jax
import jax.numpy as jnp
from jax import lax
from jax.experimental import pallas as pl
from jax.experimental.pallas import tpu as pltpu
from jax.sharding import Mesh
from jax.sharding import PartitionSpec as P

P_SIZE = 64
EPSILON = 1e-05
CHIPS = ("x", "z")
GROUP = ("x", "z", "core")
F32 = jnp.float32
BF16 = jnp.bfloat16


def from_partner(array):
    return lax.ppermute(array, "core", [(0, 1), (1, 0)])


def from_opposite(array):
    return lax.ppermute(array, "z", [(0, 1), (1, 0)])


def along_ring(array, sign):
    ring = lax.axis_size("x")
    pairs = [
        (2 * x + core, 2 * ((x + (sign if core == 0 else -sign)) % ring) + core)
        for x in range(ring)
        for core in range(2)
    ]
    return lax.ppermute(array, ("x", "core"), pairs)


def joined_kernel(in_z, in_x, in_bc, in_dt, out_t, own, sent):
    at = 0
    for part in (in_z, in_x, in_bc):
        own[:, at : at + part.shape[1]] = part[...]
        sent[:, at : at + part.shape[1]] = part[...]
        at += part.shape[1]
    heads = in_dt.shape[0]
    rows = lax.broadcasted_iota(jnp.int32, (heads, 128), 0)
    same = rows == lax.broadcasted_iota(jnp.int32, (heads, 128), 1)
    turned = lax.dot_general(
        in_dt[...], same.astype(F32).astype(BF16), (((0,), (0,)), ((), ())), preferred_element_type=F32
    )
    own[:, at : at + 128] = turned.astype(own.dtype)
    own[:, at + 128 :] = out_t[...]
    sent[:, at:] = out_t[...]


def joined(in_z, in_x, in_bc, in_dt, out_t):
    rows, inner = in_z.shape
    whole = 3 * inner + in_bc.shape[1]
    return pl.pallas_call(
        joined_kernel,
        out_shape=(
            jax.ShapeDtypeStruct((rows, whole + 128), in_z.dtype),
            jax.ShapeDtypeStruct((rows, whole), in_z.dtype),
        ),
        cost_estimate=pl.CostEstimate(flops=2000000, bytes_accessed=2 * 2 * rows * whole, transcendentals=0),
    )(in_z, in_x, in_bc, in_dt.T, out_t)


def blocks_kernel(hidden, gain, out, scale):
    values = hidden[...].astype(F32)
    mean = jnp.mean(values * values, axis=-1, keepdims=True)
    scale[...] = jnp.broadcast_to(lax.rsqrt(mean + EPSILON), scale.shape)
    gained = (values * gain[...][None, :]).astype(out.dtype)
    wide = out.shape[2] // 2
    for k in range(out.shape[0]):
        out[k, :, :wide] = gained[:, k * wide : (k + 1) * wide]
        out[k, :, wide:] = hidden[:, k * wide : (k + 1) * wide]


def hidden_blocks(hidden, gain, chips):
    seqs, width = hidden.shape
    return pl.pallas_call(
        blocks_kernel,
        out_shape=(
            jax.ShapeDtypeStruct((chips, seqs, 2 * width // chips), hidden.dtype),
            jax.ShapeDtypeStruct((seqs, 128), F32),
        ),
        cost_estimate=pl.CostEstimate(flops=1000000, bytes_accessed=300000, transcendentals=0),
    )(hidden, gain)


def placed_kernel(tags, widths, *refs):
    count = len(tags)
    pieces = refs[:count]
    outs, (held, in_sems, out_sems) = refs[-len(widths) - 3 : -3], refs[-3:]
    rows = pieces[0].shape[0]
    x, z, core = (lax.axis_index(name) for name in ("x", "z", "core"))
    reads = [
        pltpu.make_async_copy(pieces[i], held.at[i, :, pl.ds(0, pieces[i].shape[1])], in_sems.at[i])
        for i in range(count)
    ]
    for read in reads:
        read.start()
    writes = []
    for i, (turn, over, swap) in enumerate(tags):
        source_core = lax.rem(core + swap, 2)
        back = lax.rem(4 - turn + turn * 2 * source_core, 4)
        source = lax.rem(x + back, 4) * 4 + lax.rem(z + over, 2) * 2 + source_core
        at = pl.multiple_of(source * rows, rows)
        reads[i].wait()
        col = 0
        for j, wide in enumerate(widths):
            if j == len(widths) - 1:
                col = pieces[i].shape[1] - wide
            write = pltpu.make_async_copy(
                held.at[i, :, pl.ds(col, wide)],
                outs[j].at[pl.ds(at, rows), :],
                out_sems.at[i, j],
            )
            write.start()
            writes.append(write)
            col += wide
    for write in writes:
        write.wait()


def placed(pieces, devices, widths, earlier=()):
    tags, arrays = list(pieces), list(pieces.values())
    rows, whole = arrays[0].shape[0], max(a.shape[1] for a in arrays)
    count = len(tags)
    anywhere = pl.BlockSpec(memory_space=pl.ANY)
    return pl.pallas_call(
        functools.partial(placed_kernel, tags, widths),
        out_shape=tuple(jax.ShapeDtypeStruct((rows * devices, wide), arrays[0].dtype) for wide in widths),
        in_specs=[anywhere] * (count + len(earlier)),
        out_specs=tuple(anywhere for _ in widths),
        scratch_shapes=[
            pltpu.VMEM((count, rows, whole), arrays[0].dtype),
            pltpu.SemaphoreType.DMA((count,)),
            pltpu.SemaphoreType.DMA((count, len(widths))),
        ],
        input_output_aliases={count + j: j for j in range(len(earlier))},
        compiler_params=pltpu.CompilerParams(vmem_limit_bytes=12 * 2**20),
        cost_estimate=pl.CostEstimate(flops=10000000, bytes_accessed=4 * count * rows * whole, transcendentals=0),
    )(*arrays, *earlier)


def exchange(blocks, axis):
    return lax.all_to_all(blocks, axis, 0, 0, tiled=True)


def column(index, values, lanes):
    return jnp.where(lax.broadcasted_iota(jnp.int32, (values.shape[0], lanes), 1) == index, values, 0.0)


def logits_kernel(inner_total, mixed, both, gains, lm_own, lm_other, out):
    rows = lm_own.shape[0]
    vocab = lm_own.shape[1]
    core = lax.axis_index("core")
    at = lax.axis_index("x") * 4 + lax.axis_index("z") * 2 + core
    total = mixed[0].astype(F32)
    for k in range(1, mixed.shape[0]):
        total = total + mixed[k].astype(F32)
    square = total[:, 2 * rows : 2 * rows + 1] + total[:, 2 * rows + 1 : 2 * rows + 2]
    scale = lax.rsqrt(square / inner_total + EPSILON)
    left = both[:, 2 * rows : 3 * rows].astype(F32)
    right = both[:, 3 * rows : 4 * rows].astype(F32)
    stream_own = jnp.where(core == 0, left, right) + scale * total[:, :rows]
    stream_other = jnp.where(core == 0, right, left) + scale * total[:, rows : 2 * rows]
    squares = jnp.sum(stream_own * stream_own, axis=-1, keepdims=True) + jnp.sum(
        stream_other * stream_other, axis=-1, keepdims=True
    )
    final_own = (stream_own * gains[pl.ds(at, 1), :]).astype(BF16)
    final_other = (stream_other * gains[pl.ds(at + 1 - 2 * core, 1), :]).astype(BF16)
    wide = 640
    for start in range(0, vocab, wide):
        part = jnp.dot(final_own, lm_own[:, start : start + wide], preferred_element_type=F32)
        part = part + jnp.dot(final_other, lm_other[:, start : start + wide], preferred_element_type=F32)
        out[:, start : start + wide] = part.astype(BF16)
    high = squares.astype(BF16).astype(F32)
    out[:, vocab:] = (column(0, high, 128) + column(1, squares - high, 128)).astype(BF16)


def partial_logits(mixed, both, gains, lm_own, lm_other, inner_total):
    _, vocab = lm_own.shape
    return pl.pallas_call(
        functools.partial(logits_kernel, inner_total),
        out_shape=jax.ShapeDtypeStruct((both.shape[0], vocab + 128), BF16),
        compiler_params=pltpu.CompilerParams(vmem_limit_bytes=24 * 2**20),
        cost_estimate=pl.CostEstimate(flops=300000000, bytes_accessed=4000000, transcendentals=0),
    )(mixed, both, gains, lm_own, lm_other)


def stats_kernel(width, parts, reference, tokens, out):
    vocab = reference.shape[1]
    total = parts[0].astype(F32)
    for k in range(1, parts.shape[0]):
        total = total + parts[k].astype(F32)
    square = total[:, vocab : vocab + 1] + total[:, vocab + 1 : vocab + 2]
    logits = total[:, :vocab] * lax.rsqrt(square / width + EPSILON)
    rows = reference[...].astype(F32)
    columns = lax.axis_index("head") * vocab + lax.broadcasted_iota(jnp.int32, logits.shape, 1)
    picked = jnp.sum(jnp.where(columns == tokens[...], logits, 0.0), axis=-1, keepdims=True)
    roll_max = jnp.max(logits, axis=-1, keepdims=True)
    ref_max = jnp.max(rows, axis=-1, keepdims=True)
    roll_sum = jnp.sum(jnp.exp(logits - roll_max), axis=-1, keepdims=True)
    weights = jnp.exp(rows - ref_max)
    ref_sum = jnp.sum(weights, axis=-1, keepdims=True)
    cross = jnp.sum(weights * (rows - logits), axis=-1, keepdims=True)
    found = column(0, roll_max, 128)
    for index, values in enumerate((roll_sum, ref_max, ref_sum, cross, picked), 1):
        found = found + column(index, values, 128)
    turned = found.T[:8]
    for k in range(out.shape[0]):
        out[k, :, : turned.shape[1]] = turned
        out[k, :, turned.shape[1] :] = jnp.zeros((8, 128 - turned.shape[1]), F32)


def head_stats(parts, reference, tokens, width, peers):
    return pl.pallas_call(
        functools.partial(stats_kernel, width),
        out_shape=jax.ShapeDtypeStruct((peers, 8, 128), F32),
        compiler_params=pltpu.CompilerParams(vmem_limit_bytes=16 * 2**20),
        cost_estimate=pl.CostEstimate(flops=3000000, bytes_accessed=1000000, transcendentals=100000),
    )(parts, reference, tokens)


def combine_kernel(stats, divergence, logprob):
    rows = [[stats[k, j : j + 1, :] for j in range(6)] for k in range(stats.shape[0])]
    roll_top, ref_top = rows[0][0], rows[0][2]
    for row in rows[1:]:
        roll_top, ref_top = jnp.maximum(roll_top, row[0]), jnp.maximum(ref_top, row[2])
    roll_total = sum(row[1] * jnp.exp(row[0] - roll_top) for row in rows)
    scales = [jnp.exp(row[2] - ref_top) for row in rows]
    ref_total = sum(row[3] * scale for row, scale in zip(rows, scales))
    cross_total = sum(row[4] * scale for row, scale in zip(rows, scales))
    lse_roll = roll_top + jnp.log(roll_total)
    lse_ref = ref_top + jnp.log(ref_total)
    count = divergence.shape[1]
    divergence[...] = (cross_total / ref_total - lse_ref + lse_roll)[:, :count]
    logprob[...] = (sum(row[5] for row in rows) - lse_roll)[:, :count]


def combined(stats, seqs):
    return pl.pallas_call(
        combine_kernel,
        out_shape=(jax.ShapeDtypeStruct((1, seqs), F32),) * 2,
        compiler_params=pltpu.CompilerParams(vmem_limit_bytes=8 * 2**20),
        cost_estimate=pl.CostEstimate(flops=100000, bytes_accessed=40000, transcendentals=0),
    )(stats)


def input_kernel(both, own, other, out):
    rows = own.shape[0]
    core = lax.axis_index("core")
    left, right = both[:, :rows].astype(F32), both[:, rows : 2 * rows].astype(F32)
    mine = jnp.where(core == 0, left, right).astype(BF16)
    others = jnp.where(core == 0, right, left).astype(BF16)
    wide = out.shape[1] // 2 if out.shape[1] % 256 == 0 else out.shape[1]
    for start in range(0, out.shape[1], wide):
        part = jnp.dot(mine, own[:, start : start + wide], preferred_element_type=F32)
        part = part + jnp.dot(others, other[:, start : start + wide], preferred_element_type=F32)
        out[:, start : start + wide] = part.astype(BF16)


def partial_inputs(both, own, other, cols):
    return pl.pallas_call(
        input_kernel,
        out_shape=jax.ShapeDtypeStruct((both.shape[0], cols), BF16),
        compiler_params=pltpu.CompilerParams(vmem_limit_bytes=12 * 2**20),
        cost_estimate=pl.CostEstimate(flops=140000000, bytes_accessed=2000000, transcendentals=0),
    )(both, own, other)


def over_heads(values, heads):
    left = lax.broadcasted_iota(jnp.int32, (values.shape[0], 128), 1) < P_SIZE
    tiles = [
        jnp.where(left, values[:, 2 * t : 2 * t + 1], values[:, 2 * t + 1 : 2 * t + 2]) for t in range(heads // 2)
    ]
    return jnp.concatenate(tiles, axis=1)


def prepared_kernel(x_state, bc_state, taps_x, off_x, taps_bc, off_bc, dt_bias, a_log, skip, in_dt, other, out, turned):
    seqs, inner = x_state.shape[1:]
    wide = inner + bc_state.shape[2]
    for at, history, taps, offset in ((0, x_state, taps_x, off_x), (inner, bc_state, taps_bc, off_bc)):
        cols = history.shape[2]
        total = jnp.broadcast_to(offset[...][None, :], (seqs, cols))
        for k in range(3):
            total = total + history[k].astype(F32) * taps[k : k + 1, :]
        out[:seqs, at : at + cols] = total
        out[seqs : seqs + 1, at : at + cols] = taps[3:4, :]
    out[:, wide:] = jnp.zeros((out.shape[0], out.shape[1] - wide), F32)
    heads = dt_bias.shape[0]
    out[0:1, wide : wide + heads] = dt_bias[...][None, :]
    out[1:2, wide : wide + heads] = jnp.exp(a_log[...])[None, :]
    out[2:3, wide : wide + heads] = skip[...][None, :]
    turned[...] = jnp.zeros(turned.shape, turned.dtype)
    half = turned.shape[1] // 2
    rows = in_dt.shape[1]
    turned[:heads, :rows] = in_dt[...]
    turned[:, half : half + rows] = other[...].astype(F32).T[:seqs].astype(turned.dtype)


def prepared(x_state, bc_state, taps_x, off_x, taps_bc, off_bc, dt_bias, a_log, skip, in_dt, other, dt_at):
    seqs, _, inner = x_state.shape
    rows = in_dt.shape[0]
    whole = pl.BlockSpec(memory_space=pltpu.VMEM)
    return pl.pallas_call(
        prepared_kernel,
        out_shape=(
            jax.ShapeDtypeStruct((seqs + 8, inner + bc_state.shape[2] + 128), F32),
            jax.ShapeDtypeStruct((seqs, 512), BF16),
        ),
        grid=(1,),
        in_specs=[whole] * 10 + [pl.BlockSpec((rows, 128), lambda i: (0, dt_at // 128))],
        out_specs=(whole, whole),
        cost_estimate=pl.CostEstimate(flops=1000000, bytes_accessed=300000, transcendentals=0),
    )(
        x_state.transpose(1, 0, 2), bc_state.transpose(1, 0, 2), taps_x, off_x, taps_bc, off_bc,
        dt_bias, a_log, skip, in_dt.T, other,
    )


def mixer_kernel(heads, parts, scale, ready, steps, state, out, inflow, decays, b_out, held, turned, sems):
    seqs = scale.shape[0]
    inner = heads * P_SIZE
    size = state.shape[2]
    copies = [pltpu.make_async_copy(state.at[s], held.at[s], sems.at[s]) for s in range(seqs)]
    for copy in copies:
        copy.start()
    total = parts[0].astype(F32)
    for k in range(1, parts.shape[0]):
        total = total + parts[k].astype(F32)
    total = total * scale[:, :1]
    wide = inner + 2 * size
    conv = ready[:seqs, :wide] + total[:, inner : inner + wide] * ready[seqs : seqs + 1, :wide]
    conv = conv * jax.nn.sigmoid(conv)
    x_conv, b_vals, c_vals = conv[:, :inner], conv[:, inner : inner + size], conv[:, inner + size :]
    lane = lax.broadcasted_iota(jnp.int32, (inner, 128), 1)
    for s in range(seqs):
        copies[s].wait()
        sums = jnp.sum(held[s] * c_vals[s : s + 1, :], axis=-1, keepdims=True)
        if s == 0:
            turned[...] = jnp.where(lane == s, sums, 0.0)
        else:
            turned[...] = jnp.where(lane == s, sums, turned[...])
    carried = turned[...].T[:seqs]
    raw = total[:, inner + wide :] + ready[0:1, wide:]
    step = jnp.maximum(raw, 0.0) + jnp.log1p(jnp.exp(-jnp.abs(raw)))
    decay = jnp.exp(-step * ready[1:2, wide:])
    direct = step * jnp.sum(b_vals * c_vals, axis=-1, keepdims=True) + ready[2:3, wide:]
    gate = total[:, :inner]
    mixed = over_heads(decay, heads) * carried + over_heads(direct, heads) * x_conv
    mixed = (mixed * (gate * jax.nn.sigmoid(gate))).astype(out.dtype)
    for k in range(out.shape[0]):
        out[k, :, :inner] = mixed
        out[k, :, inner:] = steps[...]
    inflow[...] = over_heads(step, heads) * x_conv
    decays[...] = decay
    b_out[...] = b_vals


def mixer(parts, scale, ready, steps, state):
    chips, seqs, _ = parts.shape
    _, heads, p_size, size = state.shape
    inner = heads * p_size
    return pl.pallas_call(
        functools.partial(mixer_kernel, heads),
        out_shape=(
            jax.ShapeDtypeStruct((chips, seqs, inner + steps.shape[1]), BF16),
            jax.ShapeDtypeStruct((seqs, inner), F32),
            jax.ShapeDtypeStruct((seqs, 128), F32),
            jax.ShapeDtypeStruct((seqs, size), F32),
        ),
        in_specs=[pl.BlockSpec(memory_space=pltpu.VMEM)] * 4 + [pl.BlockSpec(memory_space=pl.ANY)],
        scratch_shapes=[
            pltpu.VMEM((seqs, inner, size), F32),
            pltpu.VMEM((inner, 128), F32),
            pltpu.SemaphoreType.DMA((seqs,)),
        ],
        compiler_params=pltpu.CompilerParams(vmem_limit_bytes=59 * 2**20),
        cost_estimate=pl.CostEstimate(flops=10000000, bytes_accessed=6000000, transcendentals=0),
    )(parts, scale, ready, steps, state.reshape(seqs, inner, size))


def mix_kernel(gated, gain, out_own, other, out, steps):
    rows, inner = out_own.shape
    heads = steps.shape[0]
    half = (gated.shape[1] - inner) // 2
    seqs = gated.shape[0] * rows * 2 // steps.shape[1]
    core = lax.axis_index("core")
    for k in range(gated.shape[0] // seqs):
        mine = gated[k * seqs : (k + 1) * seqs, inner : inner + rows].astype(F32)
        others = gated[k * seqs : (k + 1) * seqs, inner + half : inner + half + rows].astype(F32)
        left, right = jnp.where(core == 0, mine, others), jnp.where(core == 0, others, mine)
        steps[:, 2 * k * rows : (2 * k + 1) * rows] = left[:heads].astype(BF16)
        steps[:, (2 * k + 1) * rows : (2 * k + 2) * rows] = right[:heads].astype(BF16)
    values = gated[:, :inner].astype(F32)
    squares = jnp.sum(values * values, axis=-1, keepdims=True)
    gained = (values * gain[...][None, :]).astype(BF16)
    across = (((1,), (1,)), ((), ()))
    out[0, :, :rows] = lax.dot_general(gained, out_own[...], across, preferred_element_type=F32).astype(BF16)
    out[0, :, rows : 2 * rows] = lax.dot_general(
        gained, other[...], across, preferred_element_type=F32
    ).astype(BF16)
    spare = out.shape[2] - 2 * rows
    high = squares.astype(BF16).astype(F32)
    out[0, :, 2 * rows :] = (column(0, high, spare) + column(1, squares - high, spare)).astype(BF16)
    whole = out[0]
    for k in range(1, out.shape[0]):
        out[k] = whole


def partial_mix(gated, gain, out_own, other, peers, heads, width):
    rows, _ = out_own.shape
    return pl.pallas_call(
        mix_kernel,
        out_shape=(
            jax.ShapeDtypeStruct((peers, gated.shape[0], 2 * rows + 64), BF16),
            jax.ShapeDtypeStruct((heads, width), BF16),
        ),
        compiler_params=pltpu.CompilerParams(vmem_limit_bytes=12 * 2**20),
        cost_estimate=pl.CostEstimate(flops=60000000, bytes_accessed=2000000, transcendentals=0),
    )(gated, gain, out_own, other)


def shards(
    hidden_in,
    ssm_state,
    conv_x_state,
    conv_bc_state,
    token_ids,
    ref_logits,
    in_z,
    in_x,
    in_bc,
    in_dt,
    out_t,
    lm_head,
    conv_wx,
    conv_bx,
    conv_wbc,
    conv_bbc,
    dt_bias,
    a_log,
    skip_gain,
    norm_in,
    norm_gain,
    final_gain,
):
    chips = lax.axis_size(CHIPS)
    seqs, width = hidden_in.shape
    rows, inner = in_z.shape
    heads = a_log.shape[0]
    state_size = in_bc.shape[1] // 2
    class_seqs = chips * seqs

    hidden_sent, scale = hidden_blocks(hidden_in, norm_in, chips)
    full, own = joined(in_z, in_x, in_bc, in_dt, out_t)
    in_cols = full.shape[1] - inner
    dt_at = 2 * inner + 2 * state_size
    other = from_partner(full)
    ahead = along_ring(own, 1)
    behind = along_ring(own, -1)
    over = from_opposite(own)
    lm_other = from_partner(lm_head)
    far = along_ring(ahead, 1)
    ahead_z = along_ring(over, 1)
    behind_z = along_ring(over, -1)
    far_z = along_ring(ahead_z, 1)
    pieces = {(0, 0, 0): own, (0, 0, 1): other}
    for at, piece in (
        ((0, 1), over),
        ((1, 0), ahead),
        ((3, 0), behind),
        ((1, 1), ahead_z),
        ((3, 1), behind_z),
        ((2, 0), far),
        ((2, 1), far_z),
    ):
        pieces.update({(*at, 0): piece, (*at, 1): from_partner(piece)})
    widths = (inner, inner, 2 * state_size, inner)
    first, second = list(pieces)[:8], list(pieces)[8:]
    devices = 2 * chips
    rolled = placed({tag: pieces[tag] for tag in first}, devices, widths)
    rolled = placed({tag: pieces[tag] for tag in second}, devices, widths, rolled)
    roll_z, roll_x, roll_bc, roll_out = rolled

    both = exchange(hidden_sent, CHIPS)
    both = both.reshape(class_seqs, -1)

    partial_in = partial_inputs(both, full, other, in_cols).reshape(chips, seqs, in_cols)
    partial_in = exchange(partial_in, CHIPS)
    ready, steps = prepared(
        conv_x_state, conv_bc_state, conv_wx, conv_bx, conv_wbc, conv_bbc, dt_bias, a_log, skip_gain,
        in_dt, other, dt_at,
    )
    gated, inflow, decay, b_vals = mixer(partial_in, scale, ready, steps, ssm_state)
    new_state = (
        decay[:, :heads, None, None] * ssm_state
        + inflow.reshape(seqs, heads, P_SIZE)[:, :, :, None] * b_vals[:, None, None, :]
    )

    gains = final_gain.reshape(-1, rows)

    gated = exchange(gated, CHIPS)
    mix, roll_dt = partial_mix(
        gated.reshape(class_seqs, -1), norm_gain, out_t, other[:, in_cols:], lax.axis_size("head"), heads, width
    )
    roll_dt = roll_dt.T
    mix = exchange(mix, "head")

    sent = partial_logits(
        mix, both, gains, lm_head.T, lm_other.T, inner * lax.axis_size("head")
    )
    parts = exchange(sent.reshape(chips, seqs, -1), CHIPS)
    stats = head_stats(parts, ref_logits, token_ids[:, None], width, lax.axis_size("head"))
    stats = exchange(stats, "head")
    divergence, token_logprob = combined(stats, seqs)
    divergence, token_logprob = divergence[0], token_logprob[0]
    return (new_state, divergence, token_logprob, roll_z, roll_x, roll_bc, roll_dt, roll_out)


def solution(mesh):
    group, head = mesh.devices.shape
    fine = Mesh(mesh.devices.reshape(group // 4, 2, 2, head), ("x", "z", "core", "head"))
    return jax.shard_map(
        shards,
        mesh=fine,
        in_specs=(
            P(GROUP, None),
            P(GROUP, "head", None, None),
            P(GROUP, None, "head"),
            P(GROUP, None, None),
            P(GROUP),
            P(GROUP, "head"),
            P(GROUP, "head"),
            P(GROUP, "head"),
            P(GROUP, None),
            P(GROUP, "head"),
            P(GROUP, "head"),
            P("head", GROUP),
            P(None, "head"),
            P("head"),
            P(),
            P(),
            P("head"),
            P("head"),
            P("head"),
            P(),
            P("head"),
            P(),
        ),
        out_specs=(
            P(GROUP, "head", None, None),
            P(GROUP),
            P(GROUP),
            P(None, "head"),
            P(None, "head"),
            P(),
            P(None, "head"),
            P(None, "head"),
        ),
        check_vma=False,
    )
```

```python
import functools

import jax
import jax.numpy as jnp
from jax import lax
from jax.experimental import pallas as pl
from jax.experimental.pallas import tpu as pltpu
from jax.sharding import Mesh
from jax.sharding import PartitionSpec as P

P_SIZE = 64
EPSILON = 1e-05
CHIPS = ("x", "z")
GROUP = ("x", "z", "core")
F32 = jnp.float32
BF16 = jnp.bfloat16


def from_partner(array):
    return lax.ppermute(array, "core", [(0, 1), (1, 0)])


def from_opposite(array):
    return lax.ppermute(array, "z", [(0, 1), (1, 0)])


def along_ring(array, sign):
    ring = lax.axis_size("x")
    pairs = [
        (2 * x + core, 2 * ((x + (sign if core == 0 else -sign)) % ring) + core)
        for x in range(ring)
        for core in range(2)
    ]
    return lax.ppermute(array, ("x", "core"), pairs)


def joined_kernel(in_z, in_x, in_bc, in_dt, out_t, own, sent):
    at = 0
    for part in (in_z, in_x, in_bc):
        own[:, at : at + part.shape[1]] = part[...]
        sent[:, at : at + part.shape[1]] = part[...]
        at += part.shape[1]
    heads = in_dt.shape[0]
    rows = lax.broadcasted_iota(jnp.int32, (heads, 128), 0)
    same = rows == lax.broadcasted_iota(jnp.int32, (heads, 128), 1)
    turned = lax.dot_general(
        in_dt[...], same.astype(F32).astype(BF16), (((0,), (0,)), ((), ())), preferred_element_type=F32
    )
    own[:, at : at + 128] = turned.astype(own.dtype)
    own[:, at + 128 :] = out_t[...]
    sent[:, at:] = out_t[...]


def joined(in_z, in_x, in_bc, in_dt, out_t):
    rows, inner = in_z.shape
    whole = 3 * inner + in_bc.shape[1]
    return pl.pallas_call(
        joined_kernel,
        out_shape=(
            jax.ShapeDtypeStruct((rows, whole + 128), in_z.dtype),
            jax.ShapeDtypeStruct((rows, whole), in_z.dtype),
        ),
        cost_estimate=pl.CostEstimate(flops=2000000, bytes_accessed=2 * 2 * rows * whole, transcendentals=0),
    )(in_z, in_x, in_bc, in_dt.T, out_t)


def blocks_kernel(hidden, gain, out, scale):
    values = hidden[...].astype(F32)
    mean = jnp.mean(values * values, axis=-1, keepdims=True)
    scale[...] = jnp.broadcast_to(lax.rsqrt(mean + EPSILON), scale.shape)
    gained = (values * gain[...][None, :]).astype(out.dtype)
    wide = out.shape[2] // 2
    for k in range(out.shape[0]):
        out[k, :, :wide] = gained[:, k * wide : (k + 1) * wide]
        out[k, :, wide:] = hidden[:, k * wide : (k + 1) * wide]


def hidden_blocks(hidden, gain, chips):
    seqs, width = hidden.shape
    return pl.pallas_call(
        blocks_kernel,
        out_shape=(
            jax.ShapeDtypeStruct((chips, seqs, 2 * width // chips), hidden.dtype),
            jax.ShapeDtypeStruct((seqs, 128), F32),
        ),
        cost_estimate=pl.CostEstimate(flops=1000000, bytes_accessed=300000, transcendentals=0),
    )(hidden, gain)


def placed_kernel(tags, widths, *refs):
    count = len(tags)
    pieces = refs[:count]
    outs, (held, in_sems, out_sems) = refs[-len(widths) - 3 : -3], refs[-3:]
    rows = pieces[0].shape[0]
    x, z, core = (lax.axis_index(name) for name in ("x", "z", "core"))
    reads = [
        pltpu.make_async_copy(pieces[i], held.at[i, :, pl.ds(0, pieces[i].shape[1])], in_sems.at[i])
        for i in range(count)
    ]
    for read in reads:
        read.start()
    writes = []
    for i, (turn, over, swap) in enumerate(tags):
        source_core = lax.rem(core + swap, 2)
        back = lax.rem(4 - turn + turn * 2 * source_core, 4)
        source = lax.rem(x + back, 4) * 4 + lax.rem(z + over, 2) * 2 + source_core
        at = pl.multiple_of(source * rows, rows)
        reads[i].wait()
        col = 0
        for j, wide in enumerate(widths):
            if j == len(widths) - 1:
                col = pieces[i].shape[1] - wide
            write = pltpu.make_async_copy(
                held.at[i, :, pl.ds(col, wide)],
                outs[j].at[pl.ds(at, rows), :],
                out_sems.at[i, j],
            )
            write.start()
            writes.append(write)
            col += wide
    for write in writes:
        write.wait()


def placed(pieces, devices, widths, earlier=()):
    tags, arrays = list(pieces), list(pieces.values())
    rows, whole = arrays[0].shape[0], max(a.shape[1] for a in arrays)
    count = len(tags)
    anywhere = pl.BlockSpec(memory_space=pl.ANY)
    return pl.pallas_call(
        functools.partial(placed_kernel, tags, widths),
        out_shape=tuple(jax.ShapeDtypeStruct((rows * devices, wide), arrays[0].dtype) for wide in widths),
        in_specs=[anywhere] * (count + len(earlier)),
        out_specs=tuple(anywhere for _ in widths),
        scratch_shapes=[
            pltpu.VMEM((count, rows, whole), arrays[0].dtype),
            pltpu.SemaphoreType.DMA((count,)),
            pltpu.SemaphoreType.DMA((count, len(widths))),
        ],
        input_output_aliases={count + j: j for j in range(len(earlier))},
        compiler_params=pltpu.CompilerParams(vmem_limit_bytes=12 * 2**20),
        cost_estimate=pl.CostEstimate(flops=10000000, bytes_accessed=4 * count * rows * whole, transcendentals=0),
    )(*arrays, *earlier)


def exchange(blocks, axis):
    return lax.all_to_all(blocks, axis, 0, 0, tiled=True)


def column(index, values, lanes):
    return jnp.where(lax.broadcasted_iota(jnp.int32, (values.shape[0], lanes), 1) == index, values, 0.0)


def logits_kernel(inner_total, mixed, both, gains, lm_own, lm_other, out):
    rows = lm_own.shape[0]
    vocab = lm_own.shape[1]
    core = lax.axis_index("core")
    at = lax.axis_index("x") * 4 + lax.axis_index("z") * 2 + core
    total = mixed[0].astype(F32)
    for k in range(1, mixed.shape[0]):
        total = total + mixed[k].astype(F32)
    square = total[:, 2 * rows : 2 * rows + 1] + total[:, 2 * rows + 1 : 2 * rows + 2]
    scale = lax.rsqrt(square / inner_total + EPSILON)
    left = both[:, 2 * rows : 3 * rows].astype(F32)
    right = both[:, 3 * rows : 4 * rows].astype(F32)
    stream_own = jnp.where(core == 0, left, right) + scale * total[:, :rows]
    stream_other = jnp.where(core == 0, right, left) + scale * total[:, rows : 2 * rows]
    squares = jnp.sum(stream_own * stream_own, axis=-1, keepdims=True) + jnp.sum(
        stream_other * stream_other, axis=-1, keepdims=True
    )
    final_own = (stream_own * gains[pl.ds(at, 1), :]).astype(BF16)
    final_other = (stream_other * gains[pl.ds(at + 1 - 2 * core, 1), :]).astype(BF16)
    wide = 640
    for start in range(0, vocab, wide):
        part = jnp.dot(final_own, lm_own[:, start : start + wide], preferred_element_type=F32)
        part = part + jnp.dot(final_other, lm_other[:, start : start + wide], preferred_element_type=F32)
        out[:, start : start + wide] = part.astype(BF16)
    high = squares.astype(BF16).astype(F32)
    out[:, vocab:] = (column(0, high, 128) + column(1, squares - high, 128)).astype(BF16)


def partial_logits(mixed, both, gains, lm_own, lm_other, inner_total):
    _, vocab = lm_own.shape
    return pl.pallas_call(
        functools.partial(logits_kernel, inner_total),
        out_shape=jax.ShapeDtypeStruct((both.shape[0], vocab + 128), BF16),
        compiler_params=pltpu.CompilerParams(vmem_limit_bytes=24 * 2**20),
        cost_estimate=pl.CostEstimate(flops=300000000, bytes_accessed=4000000, transcendentals=0),
    )(mixed, both, gains, lm_own, lm_other)


def stats_kernel(width, parts, reference, tokens, out):
    vocab = reference.shape[1]
    total = parts[0].astype(F32)
    for k in range(1, parts.shape[0]):
        total = total + parts[k].astype(F32)
    square = total[:, vocab : vocab + 1] + total[:, vocab + 1 : vocab + 2]
    logits = total[:, :vocab] * lax.rsqrt(square / width + EPSILON)
    rows = reference[...].astype(F32)
    columns = lax.axis_index("head") * vocab + lax.broadcasted_iota(jnp.int32, logits.shape, 1)
    seqs = tokens.shape[0]
    same = lax.broadcasted_iota(jnp.int32, (seqs, seqs), 0) == lax.broadcasted_iota(jnp.int32, (seqs, seqs), 1)
    ids = jnp.sum(jnp.where(same, tokens[...].astype(F32)[None, :], 0.0), axis=-1, keepdims=True).astype(jnp.int32)
    picked = jnp.sum(jnp.where(columns == ids, logits, 0.0), axis=-1, keepdims=True)
    roll_max = jnp.max(logits, axis=-1, keepdims=True)
    ref_max = jnp.max(rows, axis=-1, keepdims=True)
    roll_sum = jnp.sum(jnp.exp(logits - roll_max), axis=-1, keepdims=True)
    weights = jnp.exp(rows - ref_max)
    ref_sum = jnp.sum(weights, axis=-1, keepdims=True)
    cross = jnp.sum(weights * (rows - logits), axis=-1, keepdims=True)
    found = column(0, roll_max, 128)
    for index, values in enumerate((roll_sum, ref_max, ref_sum, cross, picked), 1):
        found = found + column(index, values, 128)
    turned = found.T[:8]
    for k in range(out.shape[0]):
        out[k, :, : turned.shape[1]] = turned
        out[k, :, turned.shape[1] :] = jnp.zeros((8, 128 - turned.shape[1]), F32)


def head_stats(parts, reference, tokens, width, peers):
    return pl.pallas_call(
        functools.partial(stats_kernel, width),
        out_shape=jax.ShapeDtypeStruct((peers, 8, 128), F32),
        compiler_params=pltpu.CompilerParams(vmem_limit_bytes=16 * 2**20),
        cost_estimate=pl.CostEstimate(flops=3000000, bytes_accessed=1000000, transcendentals=100000),
    )(parts, reference, tokens)


def combine_kernel(stats, divergence, logprob):
    rows = [[stats[k, j : j + 1, :] for j in range(6)] for k in range(stats.shape[0])]
    roll_top, ref_top = rows[0][0], rows[0][2]
    for row in rows[1:]:
        roll_top, ref_top = jnp.maximum(roll_top, row[0]), jnp.maximum(ref_top, row[2])
    roll_total = sum(row[1] * jnp.exp(row[0] - roll_top) for row in rows)
    scales = [jnp.exp(row[2] - ref_top) for row in rows]
    ref_total = sum(row[3] * scale for row, scale in zip(rows, scales))
    cross_total = sum(row[4] * scale for row, scale in zip(rows, scales))
    lse_roll = roll_top + jnp.log(roll_total)
    lse_ref = ref_top + jnp.log(ref_total)
    count = divergence.shape[1]
    divergence[...] = (cross_total / ref_total - lse_ref + lse_roll)[:, :count]
    logprob[...] = (sum(row[5] for row in rows) - lse_roll)[:, :count]


def combined(stats, seqs):
    return pl.pallas_call(
        combine_kernel,
        out_shape=(jax.ShapeDtypeStruct((1, seqs), F32),) * 2,
        compiler_params=pltpu.CompilerParams(vmem_limit_bytes=8 * 2**20),
        cost_estimate=pl.CostEstimate(flops=100000, bytes_accessed=40000, transcendentals=0),
    )(stats)


def input_kernel(both, own, other, out):
    rows = own.shape[0]
    core = lax.axis_index("core")
    left, right = both[:, :rows].astype(F32), both[:, rows : 2 * rows].astype(F32)
    mine = jnp.where(core == 0, left, right).astype(BF16)
    others = jnp.where(core == 0, right, left).astype(BF16)
    wide = out.shape[1] // 2 if out.shape[1] % 256 == 0 else out.shape[1]
    for start in range(0, out.shape[1], wide):
        part = jnp.dot(mine, own[:, start : start + wide], preferred_element_type=F32)
        part = part + jnp.dot(others, other[:, start : start + wide], preferred_element_type=F32)
        out[:, start : start + wide] = part.astype(BF16)


def partial_inputs(both, own, other, cols):
    return pl.pallas_call(
        input_kernel,
        out_shape=jax.ShapeDtypeStruct((both.shape[0], cols), BF16),
        compiler_params=pltpu.CompilerParams(vmem_limit_bytes=12 * 2**20),
        cost_estimate=pl.CostEstimate(flops=20000000000, bytes_accessed=60000000, transcendentals=0),
    )(both, own, other)


def over_heads(values, heads):
    left = lax.broadcasted_iota(jnp.int32, (values.shape[0], 128), 1) < P_SIZE
    tiles = [
        jnp.where(left, values[:, 2 * t : 2 * t + 1], values[:, 2 * t + 1 : 2 * t + 2]) for t in range(heads // 2)
    ]
    return jnp.concatenate(tiles, axis=1)


def prepared_kernel(x_state, bc_state, taps_x, off_x, taps_bc, off_bc, dt_bias, a_log, skip, in_dt, other, out, turned):
    seqs, inner = x_state.shape[1:]
    wide = inner + bc_state.shape[2]
    for at, history, taps, offset in ((0, x_state, taps_x, off_x), (inner, bc_state, taps_bc, off_bc)):
        cols = history.shape[2]
        total = jnp.broadcast_to(offset[...][None, :], (seqs, cols))
        for k in range(3):
            total = total + history[k].astype(F32) * taps[k : k + 1, :]
        out[:seqs, at : at + cols] = total
        out[seqs : seqs + 1, at : at + cols] = taps[3:4, :]
    out[:, wide:] = jnp.zeros((out.shape[0], out.shape[1] - wide), F32)
    heads = dt_bias.shape[0]
    out[0:1, wide : wide + heads] = dt_bias[...][None, :]
    out[1:2, wide : wide + heads] = jnp.exp(a_log[...])[None, :]
    out[2:3, wide : wide + heads] = skip[...][None, :]
    turned[...] = jnp.zeros(turned.shape, turned.dtype)
    half = turned.shape[1] // 2
    rows = in_dt.shape[1]
    turned[:heads, :rows] = in_dt[...]
    turned[:, half : half + rows] = other.astype(F32).T[:seqs].astype(turned.dtype)


def mixer_kernel(
    heads, dt_at, parts, scale, x_state, bc_state, taps_x, off_x, taps_bc, off_bc, dt_bias, a_log, skip, in_dt,
    other, state, out, inflow, decays, b_out, turned, ready, steps,
):
    prepared_kernel(
        x_state, bc_state, taps_x, off_x, taps_bc, off_bc, dt_bias, a_log, skip, in_dt,
        other[:, dt_at : dt_at + 128], ready, steps,
    )
    seqs = scale.shape[0]
    inner = heads * P_SIZE
    size = state.shape[2]
    total = parts[0].astype(F32)
    for k in range(1, parts.shape[0]):
        total = total + parts[k].astype(F32)
    total = total * scale[:, :1]
    wide = inner + 2 * size
    conv = ready[:seqs, :wide] + total[:, inner : inner + wide] * ready[seqs : seqs + 1, :wide]
    conv = conv * jax.nn.sigmoid(conv)
    x_conv, b_vals, c_vals = conv[:, :inner], conv[:, inner : inner + size], conv[:, inner + size :]
    lane = lax.broadcasted_iota(jnp.int32, (inner, 128), 1)
    for s in range(seqs):
        sums = jnp.sum(state[s] * c_vals[s : s + 1, :], axis=-1, keepdims=True)
        if s == 0:
            turned[...] = jnp.where(lane == s, sums, 0.0)
        else:
            turned[...] = jnp.where(lane == s, sums, turned[...])
    carried = turned[...].T[:seqs]
    raw = total[:, inner + wide :] + ready[0:1, wide:]
    step = jnp.maximum(raw, 0.0) + jnp.log1p(jnp.exp(-jnp.abs(raw)))
    decay = jnp.exp(-step * ready[1:2, wide:])
    direct = step * jnp.sum(b_vals * c_vals, axis=-1, keepdims=True) + ready[2:3, wide:]
    gate = total[:, :inner]
    mixed = over_heads(decay, heads) * carried + over_heads(direct, heads) * x_conv
    mixed = (mixed * (gate * jax.nn.sigmoid(gate))).astype(out.dtype)
    for k in range(out.shape[0]):
        out[k, :, :inner] = mixed
        out[k, :, inner:] = steps[...]
    inflow[...] = over_heads(step, heads) * x_conv
    decays[...] = decay
    b_out[...] = b_vals


def mixer(parts, scale, vectors, in_dt, other, dt_at, state):
    chips, seqs, _ = parts.shape
    _, heads, p_size, size = state.shape
    inner = heads * p_size
    return pl.pallas_call(
        functools.partial(mixer_kernel, heads, dt_at),
        out_shape=(
            jax.ShapeDtypeStruct((chips, seqs, inner + 512), BF16),
            jax.ShapeDtypeStruct((seqs, inner), F32),
            jax.ShapeDtypeStruct((seqs, 128), F32),
            jax.ShapeDtypeStruct((seqs, size), F32),
        ),
        scratch_shapes=[
            pltpu.VMEM((inner, 128), F32),
            pltpu.VMEM((seqs + 8, inner + 2 * size + 128), F32),
            pltpu.VMEM((seqs, 512), BF16),
        ],
        compiler_params=pltpu.CompilerParams(vmem_limit_bytes=12 * 2**20),
        cost_estimate=pl.CostEstimate(flops=10000000, bytes_accessed=6000000, transcendentals=0),
    )(parts, scale, *vectors, in_dt.T, other, state.reshape(seqs, inner, size))


def mix_kernel(gated, gain, out_own, other, out, steps):
    rows, inner = out_own.shape
    heads = steps.shape[0]
    half = (gated.shape[1] - inner) // 2
    seqs = gated.shape[0] * rows * 2 // steps.shape[1]
    core = lax.axis_index("core")
    for k in range(gated.shape[0] // seqs):
        mine = gated[k * seqs : (k + 1) * seqs, inner : inner + rows].astype(F32)
        others = gated[k * seqs : (k + 1) * seqs, inner + half : inner + half + rows].astype(F32)
        left, right = jnp.where(core == 0, mine, others), jnp.where(core == 0, others, mine)
        steps[:, 2 * k * rows : (2 * k + 1) * rows] = left[:heads].astype(BF16)
        steps[:, (2 * k + 1) * rows : (2 * k + 2) * rows] = right[:heads].astype(BF16)
    values = gated[:, :inner].astype(F32)
    squares = jnp.sum(values * values, axis=-1, keepdims=True)
    gained = (values * gain[...][None, :]).astype(BF16)
    across = (((1,), (1,)), ((), ()))
    out[0, :, :rows] = lax.dot_general(gained, out_own[...], across, preferred_element_type=F32).astype(BF16)
    out[0, :, rows : 2 * rows] = lax.dot_general(
        gained, other[...], across, preferred_element_type=F32
    ).astype(BF16)
    spare = out.shape[2] - 2 * rows
    high = squares.astype(BF16).astype(F32)
    out[0, :, 2 * rows :] = (column(0, high, spare) + column(1, squares - high, spare)).astype(BF16)
    whole = out[0]
    for k in range(1, out.shape[0]):
        out[k] = whole


def partial_mix(gated, gain, out_own, other, peers, heads, width):
    rows, _ = out_own.shape
    return pl.pallas_call(
        mix_kernel,
        out_shape=(
            jax.ShapeDtypeStruct((peers, gated.shape[0], 2 * rows + 64), BF16),
            jax.ShapeDtypeStruct((heads, width), BF16),
        ),
        compiler_params=pltpu.CompilerParams(vmem_limit_bytes=12 * 2**20),
        cost_estimate=pl.CostEstimate(flops=60000000, bytes_accessed=2000000, transcendentals=0),
    )(gated, gain, out_own, other)


def shards(
    hidden_in,
    ssm_state,
    conv_x_state,
    conv_bc_state,
    token_ids,
    ref_logits,
    in_z,
    in_x,
    in_bc,
    in_dt,
    out_t,
    lm_head,
    conv_wx,
    conv_bx,
    conv_wbc,
    conv_bbc,
    dt_bias,
    a_log,
    skip_gain,
    norm_in,
    norm_gain,
    final_gain,
):
    chips = lax.axis_size(CHIPS)
    seqs, width = hidden_in.shape
    rows, inner = in_z.shape
    heads = a_log.shape[0]
    state_size = in_bc.shape[1] // 2
    class_seqs = chips * seqs

    hidden_sent, scale = hidden_blocks(hidden_in, norm_in, chips)
    full, own = joined(in_z, in_x, in_bc, in_dt, out_t)
    in_cols = full.shape[1] - inner
    dt_at = 2 * inner + 2 * state_size
    other = from_partner(full)
    ahead = along_ring(own, 1)
    behind = along_ring(own, -1)
    over = from_opposite(own)
    lm_other = from_partner(lm_head)
    far = along_ring(ahead, 1)
    ahead_z = along_ring(over, 1)
    behind_z = along_ring(over, -1)
    far_z = along_ring(ahead_z, 1)
    pieces = {(0, 0, 0): own, (0, 0, 1): other}
    for at, piece in (
        ((0, 1), over),
        ((1, 0), ahead),
        ((3, 0), behind),
        ((1, 1), ahead_z),
        ((3, 1), behind_z),
        ((2, 0), far),
        ((2, 1), far_z),
    ):
        pieces.update({(*at, 0): piece, (*at, 1): from_partner(piece)})
    widths = (inner, inner, 2 * state_size, inner)
    first, second = list(pieces)[:8], list(pieces)[8:]
    devices = 2 * chips
    rolled = placed({tag: pieces[tag] for tag in first}, devices, widths)
    rolled = placed({tag: pieces[tag] for tag in second}, devices, widths, rolled)
    roll_z, roll_x, roll_bc, roll_out = rolled

    both = exchange(hidden_sent, CHIPS)
    both = both.reshape(class_seqs, -1)

    partial_in = partial_inputs(both, full, other, in_cols).reshape(chips, seqs, in_cols)
    partial_in = exchange(partial_in, CHIPS)
    vectors = (
        conv_x_state.transpose(1, 0, 2), conv_bc_state.transpose(1, 0, 2), conv_wx, conv_bx, conv_wbc, conv_bbc,
        dt_bias, a_log, skip_gain,
    )
    gated, inflow, decay, b_vals = mixer(partial_in, scale, vectors, in_dt, other, dt_at, ssm_state)
    new_state = (
        decay[:, :heads, None, None] * ssm_state
        + inflow.reshape(seqs, heads, P_SIZE)[:, :, :, None] * b_vals[:, None, None, :]
    )

    gains = final_gain.reshape(-1, rows)

    gated = exchange(gated, CHIPS)
    mix, roll_dt = partial_mix(
        gated.reshape(class_seqs, -1), norm_gain, out_t, other[:, in_cols:], lax.axis_size("head"), heads, width
    )
    roll_dt = roll_dt.T
    mix = exchange(mix, "head")

    sent = partial_logits(
        mix, both, gains, lm_head.T, lm_other.T, inner * lax.axis_size("head")
    )
    parts = exchange(sent.reshape(chips, seqs, -1), CHIPS)
    stats = head_stats(parts, ref_logits, token_ids, width, lax.axis_size("head"))
    stats = exchange(stats, "head")
    divergence, token_logprob = combined(stats, seqs)
    divergence, token_logprob = divergence[0], token_logprob[0]
    return (new_state, divergence, token_logprob, roll_z, roll_x, roll_bc, roll_dt, roll_out)


def solution(mesh):
    group, head = mesh.devices.shape
    fine = Mesh(mesh.devices.reshape(group // 4, 2, 2, head), ("x", "z", "core", "head"))
    return jax.shard_map(
        shards,
        mesh=fine,
        in_specs=(
            P(GROUP, None),
            P(GROUP, "head", None, None),
            P(GROUP, None, "head"),
            P(GROUP, None, None),
            P(GROUP),
            P(GROUP, "head"),
            P(GROUP, "head"),
            P(GROUP, "head"),
            P(GROUP, None),
            P(GROUP, "head"),
            P(GROUP, "head"),
            P("head", GROUP),
            P(None, "head"),
            P("head"),
            P(),
            P(),
            P("head"),
            P("head"),
            P("head"),
            P(),
            P("head"),
            P(),
        ),
        out_specs=(
            P(GROUP, "head", None, None),
            P(GROUP),
            P(GROUP),
            P(None, "head"),
            P(None, "head"),
            P(),
            P(None, "head"),
            P(None, "head"),
        ),
        check_vma=False,
    )
```

```python
import functools

import jax
import jax.numpy as jnp
from jax import lax
from jax.experimental import pallas as pl
from jax.experimental.pallas import tpu as pltpu
from jax.sharding import Mesh
from jax.sharding import PartitionSpec as P

P_SIZE = 64
EPSILON = 1e-05
CHIPS = ("x", "z")
GROUP = ("x", "z", "core")
HEAD = ("y", "w")
F32 = jnp.float32
BF16 = jnp.bfloat16


def from_partner(array):
    return lax.ppermute(array, "core", [(0, 1), (1, 0)])


def from_opposite(array):
    return lax.ppermute(array, "z", [(0, 1), (1, 0)])


def along_ring(array, sign):
    ring = lax.axis_size("x")
    pairs = [
        (2 * x + core, 2 * ((x + (sign if core == 0 else -sign)) % ring) + core)
        for x in range(ring)
        for core in range(2)
    ]
    return lax.ppermute(array, ("x", "core"), pairs)


def joined_kernel(in_z, in_x, in_bc, in_dt, out_t, own, sent):
    at = 0
    for part in (in_z, in_x, in_bc):
        own[:, at : at + part.shape[1]] = part[...]
        sent[:, at : at + part.shape[1]] = part[...]
        at += part.shape[1]
    heads = in_dt.shape[0]
    rows = lax.broadcasted_iota(jnp.int32, (heads, 128), 0)
    same = rows == lax.broadcasted_iota(jnp.int32, (heads, 128), 1)
    turned = lax.dot_general(
        in_dt[...], same.astype(F32).astype(BF16), (((0,), (0,)), ((), ())), preferred_element_type=F32
    )
    own[:, at : at + 128] = turned.astype(own.dtype)
    own[:, at + 128 :] = out_t[...]
    sent[:, at:] = out_t[...]


def joined(in_z, in_x, in_bc, in_dt, out_t):
    rows, inner = in_z.shape
    whole = 3 * inner + in_bc.shape[1]
    return pl.pallas_call(
        joined_kernel,
        out_shape=(
            jax.ShapeDtypeStruct((rows, whole + 128), in_z.dtype),
            jax.ShapeDtypeStruct((rows, whole), in_z.dtype),
        ),
        cost_estimate=pl.CostEstimate(flops=2000000, bytes_accessed=2 * 2 * rows * whole, transcendentals=0),
    )(in_z, in_x, in_bc, in_dt.T, out_t)


def blocks_kernel(hidden, gain, out, scale):
    values = hidden[...].astype(F32)
    mean = jnp.mean(values * values, axis=-1, keepdims=True)
    scale[...] = jnp.broadcast_to(lax.rsqrt(mean + EPSILON), scale.shape)
    gained = (values * gain[...][None, :]).astype(out.dtype)
    wide = out.shape[2] // 2
    for k in range(out.shape[0]):
        out[k, :, :wide] = gained[:, k * wide : (k + 1) * wide]
        out[k, :, wide:] = hidden[:, k * wide : (k + 1) * wide]


def hidden_blocks(hidden, gain, chips):
    seqs, width = hidden.shape
    return pl.pallas_call(
        blocks_kernel,
        out_shape=(
            jax.ShapeDtypeStruct((chips, seqs, 2 * width // chips), hidden.dtype),
            jax.ShapeDtypeStruct((seqs, 128), F32),
        ),
        cost_estimate=pl.CostEstimate(flops=1000000, bytes_accessed=300000, transcendentals=0),
    )(hidden, gain)


def placed_kernel(tags, widths, *refs):
    count = len(tags)
    pieces = refs[:count]
    outs, (held, in_sems, out_sems) = refs[-len(widths) - 3 : -3], refs[-3:]
    rows = pieces[0].shape[0]
    x, z, core = (lax.axis_index(name) for name in ("x", "z", "core"))
    reads = [
        pltpu.make_async_copy(pieces[i], held.at[i, :, pl.ds(0, pieces[i].shape[1])], in_sems.at[i])
        for i in range(count)
    ]
    for read in reads:
        read.start()
    writes = []
    for i, (turn, over, swap) in enumerate(tags):
        source_core = lax.rem(core + swap, 2)
        back = lax.rem(4 - turn + turn * 2 * source_core, 4)
        source = lax.rem(x + back, 4) * 4 + lax.rem(z + over, 2) * 2 + source_core
        at = pl.multiple_of(source * rows, rows)
        reads[i].wait()
        col = 0
        for j, wide in enumerate(widths):
            if j == len(widths) - 1:
                col = pieces[i].shape[1] - wide
            write = pltpu.make_async_copy(
                held.at[i, :, pl.ds(col, wide)],
                outs[j].at[pl.ds(at, rows), :],
                out_sems.at[i, j],
            )
            write.start()
            writes.append(write)
            col += wide
    for write in writes:
        write.wait()


def placed(pieces, devices, widths, earlier=()):
    tags, arrays = list(pieces), list(pieces.values())
    rows, whole = arrays[0].shape[0], max(a.shape[1] for a in arrays)
    count = len(tags)
    anywhere = pl.BlockSpec(memory_space=pl.ANY)
    return pl.pallas_call(
        functools.partial(placed_kernel, tags, widths),
        out_shape=tuple(jax.ShapeDtypeStruct((rows * devices, wide), arrays[0].dtype) for wide in widths),
        in_specs=[anywhere] * (count + len(earlier)),
        out_specs=tuple(anywhere for _ in widths),
        scratch_shapes=[
            pltpu.VMEM((count, rows, whole), arrays[0].dtype),
            pltpu.SemaphoreType.DMA((count,)),
            pltpu.SemaphoreType.DMA((count, len(widths))),
        ],
        input_output_aliases={count + j: j for j in range(len(earlier))},
        compiler_params=pltpu.CompilerParams(vmem_limit_bytes=12 * 2**20),
        cost_estimate=pl.CostEstimate(flops=10000000, bytes_accessed=4 * count * rows * whole, transcendentals=0),
    )(*arrays, *earlier)


def exchange(blocks, axis):
    return lax.all_to_all(blocks, axis, 0, 0, tiled=True)


def column(index, values, lanes):
    return jnp.where(lax.broadcasted_iota(jnp.int32, (values.shape[0], lanes), 1) == index, values, 0.0)


def logits_kernel(inner_total, mixed, both, gains, lm_own, lm_other, out):
    rows = lm_own.shape[0]
    vocab = lm_own.shape[1]
    core = lax.axis_index("core")
    at = lax.axis_index("x") * 4 + lax.axis_index("z") * 2 + core
    total = mixed[0].astype(F32)
    for k in range(1, mixed.shape[0]):
        total = total + mixed[k].astype(F32)
    square = total[:, 2 * rows : 2 * rows + 1] + total[:, 2 * rows + 1 : 2 * rows + 2]
    scale = lax.rsqrt(square / inner_total + EPSILON)
    left = both[:, 2 * rows : 3 * rows].astype(F32)
    right = both[:, 3 * rows : 4 * rows].astype(F32)
    stream_own = jnp.where(core == 0, left, right) + scale * total[:, :rows]
    stream_other = jnp.where(core == 0, right, left) + scale * total[:, rows : 2 * rows]
    squares = jnp.sum(stream_own * stream_own, axis=-1, keepdims=True) + jnp.sum(
        stream_other * stream_other, axis=-1, keepdims=True
    )
    final_own = (stream_own * gains[pl.ds(at, 1), :]).astype(BF16)
    final_other = (stream_other * gains[pl.ds(at + 1 - 2 * core, 1), :]).astype(BF16)
    wide = 640
    for start in range(0, vocab, wide):
        part = jnp.dot(final_own, lm_own[:, start : start + wide], preferred_element_type=F32)
        part = part + jnp.dot(final_other, lm_other[:, start : start + wide], preferred_element_type=F32)
        out[:, start : start + wide] = part.astype(BF16)
    high = squares.astype(BF16).astype(F32)
    out[:, vocab:] = (column(0, high, 128) + column(1, squares - high, 128)).astype(BF16)


def partial_logits(mixed, both, gains, lm_own, lm_other, inner_total):
    _, vocab = lm_own.shape
    return pl.pallas_call(
        functools.partial(logits_kernel, inner_total),
        out_shape=jax.ShapeDtypeStruct((both.shape[0], vocab + 128), BF16),
        compiler_params=pltpu.CompilerParams(vmem_limit_bytes=24 * 2**20),
        cost_estimate=pl.CostEstimate(flops=300000000, bytes_accessed=4000000, transcendentals=0),
    )(mixed, both, gains, lm_own, lm_other)


def stats_kernel(width, parts, reference, tokens, out):
    vocab = reference.shape[1]
    total = parts[0].astype(F32)
    for k in range(1, parts.shape[0]):
        total = total + parts[k].astype(F32)
    square = total[:, vocab : vocab + 1] + total[:, vocab + 1 : vocab + 2]
    logits = total[:, :vocab] * lax.rsqrt(square / width + EPSILON)
    rows = reference[...].astype(F32)
    columns = (lax.axis_index("y") * 2 + lax.axis_index("w")) * vocab + lax.broadcasted_iota(jnp.int32, logits.shape, 1)
    seqs = tokens.shape[0]
    same = lax.broadcasted_iota(jnp.int32, (seqs, seqs), 0) == lax.broadcasted_iota(jnp.int32, (seqs, seqs), 1)
    ids = jnp.sum(jnp.where(same, tokens[...].astype(F32)[None, :], 0.0), axis=-1, keepdims=True).astype(jnp.int32)
    picked = jnp.sum(jnp.where(columns == ids, logits, 0.0), axis=-1, keepdims=True)
    roll_max = jnp.max(logits, axis=-1, keepdims=True)
    ref_max = jnp.max(rows, axis=-1, keepdims=True)
    roll_sum = jnp.sum(jnp.exp(logits - roll_max), axis=-1, keepdims=True)
    weights = jnp.exp(rows - ref_max)
    ref_sum = jnp.sum(weights, axis=-1, keepdims=True)
    cross = jnp.sum(weights * (rows - logits), axis=-1, keepdims=True)
    found = column(0, roll_max, 128)
    for index, values in enumerate((roll_sum, ref_max, ref_sum, cross, picked), 1):
        found = found + column(index, values, 128)
    turned = found.T[:8]
    for k in range(out.shape[0]):
        out[k, :, : turned.shape[1]] = turned
        out[k, :, turned.shape[1] :] = jnp.zeros((8, 128 - turned.shape[1]), F32)


def head_stats(parts, reference, tokens, width, peers):
    return pl.pallas_call(
        functools.partial(stats_kernel, width),
        out_shape=jax.ShapeDtypeStruct((peers, 8, 128), F32),
        compiler_params=pltpu.CompilerParams(vmem_limit_bytes=16 * 2**20),
        cost_estimate=pl.CostEstimate(flops=3000000, bytes_accessed=1000000, transcendentals=100000),
    )(parts, reference, tokens)


def combine_kernel(stats, divergence, logprob):
    rows = [[stats[k, j : j + 1, :] for j in range(6)] for k in range(stats.shape[0])]
    roll_top, ref_top = rows[0][0], rows[0][2]
    for row in rows[1:]:
        roll_top, ref_top = jnp.maximum(roll_top, row[0]), jnp.maximum(ref_top, row[2])
    roll_total = sum(row[1] * jnp.exp(row[0] - roll_top) for row in rows)
    scales = [jnp.exp(row[2] - ref_top) for row in rows]
    ref_total = sum(row[3] * scale for row, scale in zip(rows, scales))
    cross_total = sum(row[4] * scale for row, scale in zip(rows, scales))
    lse_roll = roll_top + jnp.log(roll_total)
    lse_ref = ref_top + jnp.log(ref_total)
    count = divergence.shape[1]
    divergence[...] = (cross_total / ref_total - lse_ref + lse_roll)[:, :count]
    logprob[...] = (sum(row[5] for row in rows) - lse_roll)[:, :count]


def combined(stats, seqs):
    return pl.pallas_call(
        combine_kernel,
        out_shape=(jax.ShapeDtypeStruct((1, seqs), F32),) * 2,
        compiler_params=pltpu.CompilerParams(vmem_limit_bytes=8 * 2**20),
        cost_estimate=pl.CostEstimate(flops=100000, bytes_accessed=40000, transcendentals=0),
    )(stats)


def input_kernel(both, own, other, out):
    rows = own.shape[0]
    core = lax.axis_index("core")
    left, right = both[:, :rows].astype(F32), both[:, rows : 2 * rows].astype(F32)
    mine = jnp.where(core == 0, left, right).astype(BF16)
    others = jnp.where(core == 0, right, left).astype(BF16)
    wide = out.shape[1] // 2 if out.shape[1] % 256 == 0 else out.shape[1]
    for start in range(0, out.shape[1], wide):
        part = jnp.dot(mine, own[:, start : start + wide], preferred_element_type=F32)
        part = part + jnp.dot(others, other[:, start : start + wide], preferred_element_type=F32)
        out[:, start : start + wide] = part.astype(BF16)


def partial_inputs(both, own, other, cols):
    return pl.pallas_call(
        input_kernel,
        out_shape=jax.ShapeDtypeStruct((both.shape[0], cols), BF16),
        compiler_params=pltpu.CompilerParams(vmem_limit_bytes=12 * 2**20),
        cost_estimate=pl.CostEstimate(flops=20000000000, bytes_accessed=60000000, transcendentals=0),
    )(both, own, other)


def over_heads(values, heads):
    left = lax.broadcasted_iota(jnp.int32, (values.shape[0], 128), 1) < P_SIZE
    tiles = [
        jnp.where(left, values[:, 2 * t : 2 * t + 1], values[:, 2 * t + 1 : 2 * t + 2]) for t in range(heads // 2)
    ]
    return jnp.concatenate(tiles, axis=1)


def prepared_kernel(x_state, bc_state, taps_x, off_x, taps_bc, off_bc, dt_bias, a_log, skip, in_dt, other, out, turned):
    seqs, inner = x_state.shape[1:]
    wide = inner + bc_state.shape[2]
    for at, history, taps, offset in ((0, x_state, taps_x, off_x), (inner, bc_state, taps_bc, off_bc)):
        cols = history.shape[2]
        total = jnp.broadcast_to(offset[...][None, :], (seqs, cols))
        for k in range(3):
            total = total + history[k].astype(F32) * taps[k : k + 1, :]
        out[:seqs, at : at + cols] = total
        out[seqs : seqs + 1, at : at + cols] = taps[3:4, :]
    out[:, wide:] = jnp.zeros((out.shape[0], out.shape[1] - wide), F32)
    heads = dt_bias.shape[0]
    out[0:1, wide : wide + heads] = dt_bias[...][None, :]
    out[1:2, wide : wide + heads] = jnp.exp(a_log[...])[None, :]
    out[2:3, wide : wide + heads] = skip[...][None, :]
    turned[...] = jnp.zeros(turned.shape, turned.dtype)
    half = turned.shape[1] // 2
    rows = in_dt.shape[1]
    turned[:heads, :rows] = in_dt[...]
    turned[:, half : half + rows] = other.astype(F32).T[:seqs].astype(turned.dtype)


def mixer_kernel(
    heads, dt_at, parts, scale, x_state, bc_state, taps_x, off_x, taps_bc, off_bc, dt_bias, a_log, skip, in_dt,
    other, state, out, inflow, decays, b_out, turned, ready, steps,
):
    prepared_kernel(
        x_state, bc_state, taps_x, off_x, taps_bc, off_bc, dt_bias, a_log, skip, in_dt,
        other[:, dt_at : dt_at + 128], ready, steps,
    )
    seqs = scale.shape[0]
    inner = heads * P_SIZE
    size = state.shape[2]
    total = parts[0].astype(F32)
    for k in range(1, parts.shape[0]):
        total = total + parts[k].astype(F32)
    total = total * scale[:, :1]
    wide = inner + 2 * size
    conv = ready[:seqs, :wide] + total[:, inner : inner + wide] * ready[seqs : seqs + 1, :wide]
    conv = conv * jax.nn.sigmoid(conv)
    x_conv, b_vals, c_vals = conv[:, :inner], conv[:, inner : inner + size], conv[:, inner + size :]
    lane = lax.broadcasted_iota(jnp.int32, (inner, 128), 1)
    for s in range(seqs):
        sums = jnp.sum(state[s] * c_vals[s : s + 1, :], axis=-1, keepdims=True)
        if s == 0:
            turned[...] = jnp.where(lane == s, sums, 0.0)
        else:
            turned[...] = jnp.where(lane == s, sums, turned[...])
    carried = turned[...].T[:seqs]
    raw = total[:, inner + wide :] + ready[0:1, wide:]
    step = jnp.maximum(raw, 0.0) + jnp.log1p(jnp.exp(-jnp.abs(raw)))
    decay = jnp.exp(-step * ready[1:2, wide:])
    direct = step * jnp.sum(b_vals * c_vals, axis=-1, keepdims=True) + ready[2:3, wide:]
    gate = total[:, :inner]
    mixed = over_heads(decay, heads) * carried + over_heads(direct, heads) * x_conv
    mixed = (mixed * (gate * jax.nn.sigmoid(gate))).astype(out.dtype)
    for k in range(out.shape[0]):
        out[k, :, :inner] = mixed
        out[k, :, inner:] = steps[...]
    inflow[...] = over_heads(step, heads) * x_conv
    decays[...] = decay
    b_out[...] = b_vals


def mixer(parts, scale, vectors, in_dt, other, dt_at, state):
    chips, seqs, _ = parts.shape
    _, heads, p_size, size = state.shape
    inner = heads * p_size
    return pl.pallas_call(
        functools.partial(mixer_kernel, heads, dt_at),
        out_shape=(
            jax.ShapeDtypeStruct((chips, seqs, inner + 512), BF16),
            jax.ShapeDtypeStruct((seqs, inner), F32),
            jax.ShapeDtypeStruct((seqs, 128), F32),
            jax.ShapeDtypeStruct((seqs, size), F32),
        ),
        scratch_shapes=[
            pltpu.VMEM((inner, 128), F32),
            pltpu.VMEM((seqs + 8, inner + 2 * size + 128), F32),
            pltpu.VMEM((seqs, 512), BF16),
        ],
        compiler_params=pltpu.CompilerParams(vmem_limit_bytes=12 * 2**20),
        cost_estimate=pl.CostEstimate(flops=10000000, bytes_accessed=6000000, transcendentals=0),
    )(parts, scale, *vectors, in_dt.T, other, state.reshape(seqs, inner, size))


def mix_kernel(gated, gain, out_own, other, out, steps):
    rows, inner = out_own.shape
    heads = steps.shape[0]
    half = (gated.shape[1] - inner) // 2
    seqs = gated.shape[0] * rows * 2 // steps.shape[1]
    core = lax.axis_index("core")
    for k in range(gated.shape[0] // seqs):
        mine = gated[k * seqs : (k + 1) * seqs, inner : inner + rows].astype(F32)
        others = gated[k * seqs : (k + 1) * seqs, inner + half : inner + half + rows].astype(F32)
        left, right = jnp.where(core == 0, mine, others), jnp.where(core == 0, others, mine)
        steps[:, 2 * k * rows : (2 * k + 1) * rows] = left[:heads].astype(BF16)
        steps[:, (2 * k + 1) * rows : (2 * k + 2) * rows] = right[:heads].astype(BF16)
    values = gated[:, :inner].astype(F32)
    squares = jnp.sum(values * values, axis=-1, keepdims=True)
    gained = (values * gain[...][None, :]).astype(BF16)
    across = (((1,), (1,)), ((), ()))
    out[:, :rows] = lax.dot_general(gained, out_own[...], across, preferred_element_type=F32).astype(BF16)
    out[:, rows : 2 * rows] = lax.dot_general(
        gained, other[...], across, preferred_element_type=F32
    ).astype(BF16)
    spare = out.shape[1] - 2 * rows
    high = squares.astype(BF16).astype(F32)
    out[:, 2 * rows :] = (column(0, high, spare) + column(1, squares - high, spare)).astype(BF16)


def folded_kernel(at, mine, others, out):
    total = mine[...].astype(F32) + others[...].astype(F32)
    squares = total[:, at : at + 1] + total[:, at + 1 : at + 2]
    high = squares.astype(BF16).astype(F32)
    lane = lax.broadcasted_iota(jnp.int32, total.shape, 1)
    total = jnp.where(lane == at, high, jnp.where(lane == at + 1, squares - high, total)).astype(BF16)
    for k in range(out.shape[0]):
        out[k] = total


def folded(mine, others, at, peers):
    return pl.pallas_call(
        functools.partial(folded_kernel, at),
        out_shape=jax.ShapeDtypeStruct((peers, *mine.shape), BF16),
        compiler_params=pltpu.CompilerParams(vmem_limit_bytes=8 * 2**20),
        cost_estimate=pl.CostEstimate(flops=1000000, bytes_accessed=600000, transcendentals=0),
    )(mine, others)


def partial_mix(gated, gain, out_own, other, heads, width):
    rows, _ = out_own.shape
    return pl.pallas_call(
        mix_kernel,
        out_shape=(
            jax.ShapeDtypeStruct((gated.shape[0], 2 * rows + 64), BF16),
            jax.ShapeDtypeStruct((heads, width), BF16),
        ),
        compiler_params=pltpu.CompilerParams(vmem_limit_bytes=12 * 2**20),
        cost_estimate=pl.CostEstimate(flops=60000000, bytes_accessed=2000000, transcendentals=0),
    )(gated, gain, out_own, other)


def shards(
    hidden_in,
    ssm_state,
    conv_x_state,
    conv_bc_state,
    token_ids,
    ref_logits,
    in_z,
    in_x,
    in_bc,
    in_dt,
    out_t,
    lm_head,
    conv_wx,
    conv_bx,
    conv_wbc,
    conv_bbc,
    dt_bias,
    a_log,
    skip_gain,
    norm_in,
    norm_gain,
    final_gain,
):
    chips = lax.axis_size(CHIPS)
    seqs, width = hidden_in.shape
    rows, inner = in_z.shape
    heads = a_log.shape[0]
    state_size = in_bc.shape[1] // 2
    class_seqs = chips * seqs

    hidden_sent, scale = hidden_blocks(hidden_in, norm_in, chips)
    full, own = joined(in_z, in_x, in_bc, in_dt, out_t)
    in_cols = full.shape[1] - inner
    dt_at = 2 * inner + 2 * state_size
    other = from_partner(full)
    ahead = along_ring(own, 1)
    behind = along_ring(own, -1)
    over = from_opposite(own)
    lm_other = from_partner(lm_head)
    far = along_ring(ahead, 1)
    ahead_z = along_ring(over, 1)
    behind_z = along_ring(over, -1)
    far_z = along_ring(ahead_z, 1)
    pieces = {(0, 0, 0): own, (0, 0, 1): other}
    for at, piece in (
        ((0, 1), over),
        ((1, 0), ahead),
        ((3, 0), behind),
        ((1, 1), ahead_z),
        ((3, 1), behind_z),
        ((2, 0), far),
        ((2, 1), far_z),
    ):
        pieces.update({(*at, 0): piece, (*at, 1): from_partner(piece)})
    widths = (inner, inner, 2 * state_size, inner)
    first, second = list(pieces)[:8], list(pieces)[8:]
    devices = 2 * chips
    rolled = placed({tag: pieces[tag] for tag in first}, devices, widths)
    rolled = placed({tag: pieces[tag] for tag in second}, devices, widths, rolled)
    roll_z, roll_x, roll_bc, roll_out = rolled

    both = exchange(hidden_sent, CHIPS)
    both = both.reshape(class_seqs, -1)

    partial_in = partial_inputs(both, full, other, in_cols).reshape(chips, seqs, in_cols)
    partial_in = exchange(partial_in, CHIPS)
    vectors = (
        conv_x_state.transpose(1, 0, 2), conv_bc_state.transpose(1, 0, 2), conv_wx, conv_bx, conv_wbc, conv_bbc,
        dt_bias, a_log, skip_gain,
    )
    gated, inflow, decay, b_vals = mixer(partial_in, scale, vectors, in_dt, other, dt_at, ssm_state)
    new_state = (
        decay[:, :heads, None, None] * ssm_state
        + inflow.reshape(seqs, heads, P_SIZE)[:, :, :, None] * b_vals[:, None, None, :]
    )

    gains = final_gain.reshape(-1, rows)

    gated = exchange(gated, CHIPS)
    mix, roll_dt = partial_mix(
        gated.reshape(class_seqs, -1), norm_gain, out_t, other[:, in_cols:], heads, width
    )
    roll_dt = roll_dt.T
    mix_pair = lax.ppermute(mix, "w", [(0, 1), (1, 0)])
    mix = folded(mix, mix_pair, 2 * rows, lax.axis_size("y"))
    mix = exchange(mix, "y")

    sent = partial_logits(
        mix, both, gains, lm_head.T, lm_other.T, inner * lax.axis_size(HEAD)
    )
    parts = exchange(sent.reshape(chips, seqs, -1), CHIPS)
    stats = head_stats(parts, ref_logits, token_ids, width, lax.axis_size(HEAD))
    stats = exchange(stats, HEAD)
    divergence, token_logprob = combined(stats, seqs)
    divergence, token_logprob = divergence[0], token_logprob[0]
    return (new_state, divergence, token_logprob, roll_z, roll_x, roll_bc, roll_dt, roll_out)


def solution(mesh):
    group, head = mesh.devices.shape
    fine = Mesh(mesh.devices.reshape(group // 4, 2, 2, head // 2, 2), ("x", "z", "core", "y", "w"))
    return jax.shard_map(
        shards,
        mesh=fine,
        in_specs=(
            P(GROUP, None),
            P(GROUP, HEAD, None, None),
            P(GROUP, None, HEAD),
            P(GROUP, None, None),
            P(GROUP),
            P(GROUP, HEAD),
            P(GROUP, HEAD),
            P(GROUP, HEAD),
            P(GROUP, None),
            P(GROUP, HEAD),
            P(GROUP, HEAD),
            P(HEAD, GROUP),
            P(None, HEAD),
            P(HEAD),
            P(),
            P(),
            P(HEAD),
            P(HEAD),
            P(HEAD),
            P(),
            P(HEAD),
            P(),
        ),
        out_specs=(
            P(GROUP, HEAD, None, None),
            P(GROUP),
            P(GROUP),
            P(None, HEAD),
            P(None, HEAD),
            P(),
            P(None, HEAD),
            P(None, HEAD),
        ),
        check_vma=False,
    )
```
